32 devices in a mesh: grp: 4 (over z), loc: 8 (over y, x, core).
Axes of the slice: x: 2, y: 2, z: 4, core: 2. Of those that a mesh axis runs over, the one named last changes fastest.
Arguments:
- features: float32 [32768, 256], P(('grp', 'loc')), may hold values from -6 to 6
- hub_block: bfloat16 [128, 32768], P(None, ('grp', 'loc')), may hold values from -0.0625 to 0.0625
- hub_slot: int32 [128], P(('grp', 'loc')), may hold values from 0 to 1023, as said below
- neighbours: int32 [32768, 16], P(('grp', 'loc')), may hold values from 0 to 2047
- counts: int32 [32768], P(('grp', 'loc')), may hold values from 1 to 16
- halo_send: int32 [256, 128], P(('grp', 'loc')), may hold values from 0 to 1023
- weight: float32 [256, 256], replicated, may hold values from -0.375 to 0.375
- bias: float32 [256], replicated, may hold values from -3 to 3
Outputs:
- layer_out: float32 [32768, 256], P(('grp', 'loc'))
The draws below stay inside these ranges and needn't reach their ends.
Inputs may be any that keep to these rules, and one draw needn't show every extreme that they name: `hub_slot`: within each aligned block of 4 entries the values are distinct.
All inputs are finite; a program needn't handle non-finite values.
Results may differ from the reference program's by a relative error of at most 0.0003.
Values sent between devices are 32-bit elements; how exact they have to be, the bound alone decides.
A program may use at most 64 MiB of HBM per device.

```python
import jax
import jax.numpy as jnp
from jax import lax

F = 256
V_DEV = 1024
HUB_DEV = 4
K = 16
S = 128
V = 32768
HUB = 128
N_GRP = 4
N_LOC = 8
DEVICES = 32


def draw_hub_slot(key, part):
    owners = HUB // HUB_DEV
    keys = jax.random.split(jax.random.fold_in(key, 11), owners)
    picked = jax.vmap(lambda single: jax.random.permutation(single, V_DEV)[:HUB_DEV])(keys)
    return picked.reshape(-1).astype(jnp.int32)


def place_ends(array, stream_key, least, largest):
    shape = array.shape
    spot = [jax.random.randint(jax.random.fold_in(stream_key, axis), (), 0, shape[axis]) for axis in range(len(shape))]
    array = array.at[tuple(spot)].set(least)
    longest = shape.index(max(shape))
    spot[longest] = (spot[longest] + 1) % shape[longest]
    return array.at[tuple(spot)].set(largest)


def spiked(entries, own_key, source, target, blocks, factor):
    def block_of(position):
        return (jnp.arange(entries.shape[position]) // (entries.shape[position] // blocks)).reshape((-1,) + (1,) * (entries.ndim - 1 - position))

    first = jax.random.permutation(own_key, blocks)[block_of(target)]
    other_side = (block_of(target) + blocks // 2) % blocks
    return jnp.where((block_of(source) == first) | (block_of(source) == other_side), factor * entries, entries)


def block_levels(key, extent, cuts, low, top_value):
    def one(dim, shards_of):
        draws = jax.random.uniform(jax.random.fold_in(jax.random.fold_in(key, 6), dim), (shards_of,), jnp.float32, low / len(cuts), top_value / len(cuts))
        return jnp.repeat(jnp.exp(draws), extent[dim] // shards_of).reshape((-1,) + (1,) * (len(extent) - dim - 1))

    loudness = one(*cuts[0])
    for cut in cuts[1:]:
        loudness = loudness * one(*cut)
    return loudness


def centred(key, extent, width, bound, cuts=(), kind=jnp.bfloat16):
    array = jax.random.normal(key, extent, jnp.float32) * width
    if len(cuts) > 0:
        array = block_levels(key, extent, cuts, -0.22, 0.18) * array
    return jnp.clip(array, min=-bound, max=bound).astype(kind)


def heavy_noise(key, extent, deviation, most, cuts, heavy, kind=jnp.bfloat16):
    entries = deviation * jax.random.normal(key, extent, jnp.float32)
    if cuts:
        entries = entries * block_levels(key, extent, cuts, -0.22, 0.18)
    return jnp.clip(spiked(entries, jax.random.fold_in(key, 3), *heavy), -most, most).astype(kind)


def setup_inputs(seed: int = 0) -> dict:
    splits = jax.random.split(jax.random.key(seed), 9)
    return {
        "features": centred(splits[0], (V, F), 1.0, 6.0, ((0, 32),), jnp.float32),
        "hub_block": heavy_noise(splits[1], (HUB, V), V ** -0.5, 0.0625, ((1, 32),), (1, 0, 32, 2.75)),
        "hub_slot": draw_hub_slot(jax.random.fold_in(splits[8], 71), 0),
        "neighbours": place_ends(jax.random.randint(splits[3], (V, K), 0, V_DEV + N_LOC * S), jax.random.fold_in(splits[3], 1), 0, (V_DEV + N_LOC * S) - 1).astype(jnp.int32),
        "counts": place_ends(jax.random.randint(splits[4], (V,), 1, K + 1), jax.random.fold_in(splits[4], 1), 1, K).astype(jnp.int32),
        "halo_send": place_ends(jax.random.randint(splits[5], (DEVICES * N_LOC, S), 0, V_DEV), jax.random.fold_in(splits[5], 1), 0, V_DEV - 1).astype(jnp.int32),
        "weight": centred(splits[6], (F, F), F ** -0.5, 0.375, (), jnp.float32),
        "bias": centred(splits[7], (F,), 0.5, 3.0, (), jnp.float32),
    }


def reference(features, hub_block, hub_slot, neighbours, counts, halo_send, weight, bias):
    rounded = features.astype(jnp.bfloat16)
    hub_sum = jnp.dot(hub_block, rounded, preferred_element_type=jnp.float32)
    devices = N_GRP * N_LOC
    send_table = halo_send.reshape(devices, N_LOC, S)
    nbr_blocks = neighbours.reshape(devices, V_DEV, K)
    cnt_blocks = counts.reshape(devices, V_DEV)

    def one_device(device):
        group = device // N_LOC
        place = device % N_LOC
        peers = (group * N_LOC + jnp.arange(N_LOC)).astype(jnp.int32)
        sent_rows = send_table[peers, place]
        remote_ids = (peers[:, None] * V_DEV + sent_rows).reshape(-1)
        own_ids = (device * V_DEV + jnp.arange(V_DEV)).astype(jnp.int32)
        ids_table = jnp.concatenate([own_ids, remote_ids.astype(jnp.int32)])
        slots = nbr_blocks[device]
        gathered = features[ids_table[slots]]
        used = (jnp.arange(K)[None, :] < cnt_blocks[device][:, None]).astype(jnp.float32)
        summed = jnp.sum(gathered * used[:, :, None], axis=1)
        return summed / cnt_blocks[device].astype(jnp.float32)[:, None]

    low = lax.map(one_device, jnp.arange(devices).astype(jnp.int32)).reshape(-1, F)
    combined = features + low
    targets = (jnp.arange(HUB) // HUB_DEV).astype(jnp.int32) * V_DEV + hub_slot
    combined = combined.at[targets].add(hub_sum)
    result = jnp.dot(combined, weight, precision=lax.Precision.HIGHEST, preferred_element_type=jnp.float32) + bias
    return jnp.maximum(result, 0.0)
```

```python
import functools

import jax
import jax.numpy as jnp
from jax import lax
from jax.experimental import pallas as pl
from jax.experimental.pallas import tpu as pltpu
from jax.sharding import PartitionSpec as P

BF = jnp.bfloat16
F32 = jnp.float32
LANES = 128


def flip(index, mask, count):
    result = index
    bit = 1
    while bit < count:
        if mask & bit:
            result = result + bit * (1 - 2 * ((index // bit) % 2))
        bit *= 2
    return result


def send_order(count):
    near = [off for off in range(2, count) if bin(off >> 1).count("1") == 1]
    far = [off for off in range(2, count) if bin(off >> 1).count("1") > 1]
    near.sort(key=lambda off: (off & 1, off))
    return near[:2] + [1] + near[2:] + far


def dot(a, b):
    return jnp.dot(a, b, preferred_element_type=F32)


def dot_nt(a, b):
    return lax.dot_general(a, b, (((1,), (1,)), ((), ())), preferred_element_type=F32)


def split(x):
    high = x.astype(BF)
    return high, (x - high.astype(F32)).astype(BF)


def onehot(mask):
    return jnp.where(mask, 1.0, 0.0).astype(BF)


def iota(shape, dim):
    return lax.broadcasted_iota(jnp.int32, shape, dim)


def kernel(
    n_grp, n_loc,
    feat_hbm, hub_hbm, slot_hbm, nbr_hbm, cnt_hbm, halo_hbm, w_hbm, bias_hbm,
    out_ref,
    feat_ref, hub_ref, slot_ref, nbr_ref, cnt_ref, halo_ref, w_ref, bias_ref, loaded,
    go, fh, ph, pl_, prod, base, acc, adj_own, adj, codes, lows, outgoing, recv, part, part_in, spread, spread_in,
    inv, wh, wl,
    halo_s, halo_r, grp_s, grp_r, loc_s, loc_r,
):
    grp = lax.axis_index("grp")
    me = lax.axis_index("loc")
    rows, width = feat_ref.shape
    listed = halo_ref.shape[1]
    slots = nbr_ref.shape[0]
    hub_grp = hub_ref.shape[0] // n_grp
    hub_dev = slot_ref.shape[0]
    levels = rows // LANES + n_loc * listed // LANES
    per_block = 256 // slots
    blocks = rows // per_block

    barrier = pltpu.get_barrier_semaphore()
    for off in range(1, n_loc):
        pl.semaphore_signal(
            barrier, inc=1, device_id={"loc": flip(me, off, n_loc)}, device_id_type=pl.DeviceIdType.MESH
        )

    halo_load, feat_load, hub_load, nbr_load, cnt_load, w_load, bias_load, slot_load = [
        pltpu.make_async_copy(source, target, loaded.at[number])
        for number, (source, target) in enumerate((
            (halo_hbm, halo_ref), (feat_hbm, feat_ref), (hub_hbm, hub_ref), (nbr_hbm, nbr_ref),
            (cnt_hbm, cnt_ref), (w_hbm, w_ref), (bias_hbm, bias_ref), (slot_hbm, slot_ref),
        ))
    ]
    for load in (halo_load, feat_load, w_load, bias_load, hub_load, nbr_load, cnt_load, slot_load):
        load.start()

    def times_weight(x_high, x_low):
        return dot(x_high, wh[...]) + dot(x_low, wh[...]) + dot(x_high, wl[...])

    chunk = 16

    def gather(source, peer, target, start):
        def rows_of(step, carry):
            for inner in range(chunk):
                row = step * chunk + inner
                target[pl.ds(start + row, 1), :] = source[pl.ds(halo_ref[peer, row], 1), :]
            return carry

        lax.fori_loop(0, listed // chunk, rows_of, 0)

    def halo_copy(off):
        return pltpu.make_async_remote_copy(
            src_ref=outgoing.at[off],
            dst_ref=recv.at[pl.ds(pl.multiple_of(me * listed, listed), listed)],
            send_sem=halo_s.at[off],
            recv_sem=halo_r.at[off],
            device_id={"loc": flip(me, off, n_loc)},
            device_id_type=pl.DeviceIdType.MESH,
        )

    def grp_copy(off):
        target = (grp + off) % n_grp
        return pltpu.make_async_remote_copy(
            src_ref=part.at[pl.ds(pl.multiple_of(target * hub_grp, hub_grp), hub_grp)],
            dst_ref=part_in.at[off],
            send_sem=grp_s.at[off],
            recv_sem=grp_r.at[off],
            device_id={"grp": target},
            device_id_type=pl.DeviceIdType.MESH,
        )

    def loc_copy(off):
        target = flip(me, off, n_loc)
        return pltpu.make_async_remote_copy(
            src_ref=spread.at[target],
            dst_ref=spread_in.at[off],
            send_sem=loc_s.at[off],
            recv_sem=loc_r.at[off],
            device_id={"loc": target},
            device_id_type=pl.DeviceIdType.MESH,
        )

    order = send_order(n_loc)
    early, late, held = order[:2], order[2:-1], order[-1]

    halo_load.wait()
    feat_load.wait()
    gather(feat_ref, flip(me, early[0], n_loc), outgoing.at[early[0]], 0)

    pl.semaphore_wait(barrier, n_loc - 1 + jnp.where(me == 1, n_grp - 1, 0))

    @pl.when(me == 0)
    def _():
        for off in range(1, n_grp):
            pl.semaphore_signal(
                barrier, inc=1, device_id={"grp": (grp + off) % n_grp, "loc": 1},
                device_id_type=pl.DeviceIdType.MESH,
            )

    @pl.when(me == 1)
    def _():
        for off in range(1, n_loc):
            pl.semaphore_signal(
                go, inc=1, device_id={"loc": flip(me, off, n_loc)}, device_id_type=pl.DeviceIdType.MESH
            )
        pl.semaphore_signal(go, inc=1)

    halo_copy(early[0]).start()
    for off in early[1:]:
        gather(feat_ref, flip(me, off, n_loc), outgoing.at[off], 0)
        halo_copy(off).start()

    w_load.wait()
    w_high, w_low = split(w_ref[...])
    wh[...] = w_high
    wl[...] = w_low
    high, low = split(feat_ref[...])
    fh[...] = high
    product = times_weight(high, low)
    prod[...] = product
    p_high, p_low = split(product)
    ph[...] = p_high
    pl_[...] = p_low

    for off in late:
        gather(prod, flip(me, off, n_loc), outgoing.at[off], 0)
        halo_copy(off).start()
    gather(prod, flip(me, held, n_loc), outgoing.at[held], 0)
    gather(prod, me, recv, pl.multiple_of(me * listed, listed))

    hub_load.wait()
    part[...] = dot(hub_ref[...], fh[...])

    nbr_load.wait()
    cnt_load.wait()
    slot = nbr_ref[...]
    used = iota((slots, rows), 0) < jnp.broadcast_to(cnt_ref[...], (slots, rows))
    level = jnp.where(used, lax.shift_right_logical(slot, 7), -16).astype(F32)
    place = jnp.where(used, slot & (LANES - 1), 0).astype(F32)
    spots = (iota((rows, 256), 0) % per_block) == (iota((rows, 256), 1) % per_block)
    repeat = onehot(iota((slots, 256), 1) // per_block == iota((slots, 256), 0))
    member = onehot(iota((blocks, rows), 1) // per_block == iota((blocks, rows), 0))

    def flatten(table):
        spread_out = dot(jnp.transpose(table).astype(BF), repeat)
        return dot(member, jnp.where(spots, spread_out, 0.0).astype(BF))

    codes[...] = flatten(level).astype(jnp.int32) * per_block + iota((blocks, 256), 1) % per_block
    lows[...] = flatten(place).astype(jnp.int32)
    inv[...] = 1.0 / jnp.transpose(jnp.broadcast_to(cnt_ref[...].astype(F32), (8, rows)))

    group = 4
    own = rows // 256

    def build(step, carry):
        for inner in range(group):
            block = step * group + inner
            code = codes[pl.ds(block, 1), :]
            spot = lows[pl.ds(block, 1), :]
            left = onehot(iota((levels * per_block, 256), 0) == code)
            right = onehot(iota((LANES, 256), 0) == spot)
            counted = dot_nt(left, right).astype(BF)
            at = pl.ds(pl.multiple_of(block * per_block, per_block), per_block)
            for tile in range(levels):
                piece = counted[tile * per_block:(tile + 1) * per_block]
                if tile < 2 * own:
                    adj_own[at, tile * LANES:(tile + 1) * LANES] = piece
                else:
                    adj[tile - 2 * own, at, 0:LANES] = piece
                    adj[tile - 2 * own, at, LANES:2 * LANES] = piece
        return carry

    half = blocks // group // 2
    lax.fori_loop(0, half, build, 0)
    pl.semaphore_wait(go, 1)
    for off in range(1, n_grp):
        grp_copy(off).start()
    lax.fori_loop(half, blocks // group, build, 0)

    for off in range(1, n_grp):
        grp_copy(off).wait_recv()
    group_sum = part[pl.ds(pl.multiple_of(grp * hub_grp, hub_grp), hub_grp), :]
    for off in range(1, n_grp):
        group_sum = group_sum + part_in[off]
    if 2 * hub_dev < spread.shape[1]:
        spread[...] = jnp.zeros_like(spread)
    for owner in range(n_loc):
        own_rows = group_sum[owner * hub_dev:(owner + 1) * hub_dev]
        spread[owner, 0:hub_dev, :] = own_rows[:, 0:width // 2]
        spread[owner, hub_dev:2 * hub_dev, :] = own_rows[:, width // 2:]
    for off in range(1, n_loc):
        loc_copy(off).start()
    halo_copy(held).start()

    acc[...] = dot(adj_own[...], ph[...]) + dot(adj_own[...], pl_[...])

    def take(off):
        peer = flip(me, off, n_loc)
        got = recv[pl.ds(pl.multiple_of(peer * listed, listed), listed), :]
        if off in early:
            got = times_weight(*split(got))
        r_high, r_low = split(got)
        return dot(adj[peer], jnp.concatenate([r_high, r_low], axis=0))

    acc[...] += take(0)
    for off in [1] + early + late[1:]:
        halo_copy(off).wait_recv()
        acc[...] += take(off)

    hubs = spread[me]
    for off in range(1, n_loc):
        loc_copy(off).wait_recv()
        hubs = hubs + spread_in[off]
    hubs = jnp.concatenate([hubs[0:hub_dev], hubs[hub_dev:2 * hub_dev]], axis=1)
    hubs = jnp.concatenate([hubs, jnp.zeros((LANES - hub_dev, width), F32)], axis=0)
    h_high, h_low = split(times_weight(*split(hubs)))
    slot_load.wait()
    bias_load.wait()
    lane = iota((1, LANES), 1)
    target_row = jnp.full((1, LANES), -1, jnp.int32)
    for hub in range(hub_dev):
        target_row = jnp.where(lane == hub, slot_ref[hub], target_row)
    here = onehot(iota((rows, LANES), 0) == target_row)
    base[...] = prod[...] + bias_ref[...] + dot(here, h_high) + dot(here, h_low)

    halo_copy(held).wait_recv()
    out_ref[...] = jnp.maximum((acc[...] + take(held)) * inv[:, 0:1] + base[...], 0.0)

    for off in range(1, n_loc):
        halo_copy(off).wait_send()
        loc_copy(off).wait_send()
    for off in range(1, n_grp):
        grp_copy(off).wait_send()


def solution(mesh):
    n_grp, n_loc = mesh.shape["grp"], mesh.shape["loc"]

    def on_device(features, hub_block, hub_slot, neighbours, counts, halo_send, weight, bias):
        rows, width = features.shape
        slots = neighbours.shape[1]
        listed = halo_send.shape[1]
        hubs = hub_block.shape[0]
        blocks = rows // (256 // slots)
        padded = -(-2 * hub_slot.shape[0] // 8) * 8
        vmem = pl.BlockSpec(memory_space=pltpu.VMEM)
        far = pl.BlockSpec(memory_space=pltpu.HBM)
        sem = pltpu.SemaphoreType.DMA
        return pl.pallas_call(
            functools.partial(kernel, n_grp, n_loc),
            out_shape=jax.ShapeDtypeStruct((rows, width), F32),
            in_specs=[far] * 8,
            out_specs=vmem,
            scratch_shapes=[
                pltpu.VMEM(features.shape, F32),
                pltpu.VMEM(hub_block.shape, BF),
                pltpu.SMEM(hub_slot.shape, jnp.int32),
                pltpu.VMEM((slots, rows), jnp.int32),
                pltpu.VMEM((1, rows), jnp.int32),
                pltpu.SMEM(halo_send.shape, jnp.int32),
                pltpu.VMEM(weight.shape, F32),
                pltpu.VMEM((1, width), F32),
                sem((8,)),
                pltpu.SemaphoreType.REGULAR,
                pltpu.VMEM((rows, width), BF),
                pltpu.VMEM((rows, width), BF),
                pltpu.VMEM((rows, width), BF),
                pltpu.VMEM((rows, width), F32),
                pltpu.VMEM((rows, width), F32),
                pltpu.VMEM((rows, width), F32),
                pltpu.VMEM((rows, rows), BF),
                pltpu.VMEM((n_loc, rows, 256), BF),
                pltpu.VMEM((blocks, 256), jnp.int32),
                pltpu.VMEM((blocks, 256), jnp.int32),
                pltpu.VMEM((n_loc, listed, width), F32),
                pltpu.VMEM((n_loc * listed, width), F32),
                pltpu.VMEM((hubs, width), F32),
                pltpu.VMEM((n_grp, hubs // n_grp, width), F32),
                pltpu.VMEM((n_loc, padded, width // 2), F32),
                pltpu.VMEM((n_loc, padded, width // 2), F32),
                pltpu.VMEM((rows, 8), F32),
                pltpu.VMEM(weight.shape, BF),
                pltpu.VMEM(weight.shape, BF),
                sem((n_loc,)), sem((n_loc,)), sem((n_grp,)), sem((n_grp,)), sem((n_loc,)), sem((n_loc,)),
            ],
            compiler_params=pltpu.CompilerParams(
                collective_id=0, has_side_effects=True, vmem_limit_bytes=48 * 1024 * 1024
            ),
        )(
            *[
                pltpu.with_memory_space_constraint(array, pltpu.HBM)
                for array in (
                    features, hub_block, hub_slot, neighbours.T, counts.reshape(1, -1), halo_send, weight,
                    bias.reshape(1, -1),
                )
            ]
        )

    both = ("grp", "loc")
    return jax.shard_map(
        on_device,
        mesh=mesh,
        in_specs=(P(both, None), P(None, both), P(both), P(both, None), P(both), P(both, None), P(), P()),
        out_specs=P(both, None),
        check_vma=False,
    )
```

```python
import functools

import jax
import jax.numpy as jnp
from jax import lax
from jax.experimental import pallas as pl
from jax.experimental.pallas import tpu as pltpu
from jax.sharding import PartitionSpec as P

BF = jnp.bfloat16
F32 = jnp.float32
LANES = 128


def flip(index, mask, count):
    result = index
    bit = 1
    while bit < count:
        if mask & bit:
            result = result + bit * (1 - 2 * ((index // bit) % 2))
        bit *= 2
    return result


def send_order(count):
    near = [off for off in range(2, count) if bin(off >> 1).count("1") == 1]
    far = [off for off in range(2, count) if bin(off >> 1).count("1") > 1]
    near.sort(key=lambda off: (off & 1, off))
    return near[:2] + [1] + near[2:] + far


def dot(a, b):
    return jnp.dot(a, b, preferred_element_type=F32)


def dot_nt(a, b):
    return lax.dot_general(a, b, (((1,), (1,)), ((), ())), preferred_element_type=F32)


def split(x):
    high = x.astype(BF)
    return high, (x - high.astype(F32)).astype(BF)


def onehot(mask):
    return jnp.where(mask, 1.0, 0.0).astype(BF)


def iota(shape, dim):
    return lax.broadcasted_iota(jnp.int32, shape, dim)


def kernel(
    n_grp, n_loc,
    feat_hbm, hub_hbm, slot_hbm, nbr_hbm, cnt_hbm, halo_hbm, w_hbm, bias_hbm,
    out_ref,
    feat_ref, hub_ref, slot_ref, nbr_ref, cnt_ref, halo_ref, w_ref, bias_ref, loaded,
    go, fh, ph, pl_, prod, table, base, acc, adj_own, adj, codes, lows, outgoing, recv, part, part_in, spread, spread_in,
    inv, wh, wl,
    halo_s, halo_r, grp_s, grp_r, loc_s, loc_r,
):
    grp = lax.axis_index("grp")
    me = lax.axis_index("loc")
    rows, width = feat_hbm.shape
    chunk = outgoing.shape[3]
    listed = outgoing.shape[2] * chunk
    slots = nbr_ref.shape[0]
    hub_grp = hub_ref.shape[0] // n_grp
    hub_dev = slot_ref.shape[0]
    levels = rows // LANES + n_loc * listed // LANES
    per_block = 256 // slots
    blocks = rows // per_block

    barrier = pltpu.get_barrier_semaphore()
    for off in range(1, n_loc):
        pl.semaphore_signal(
            barrier, inc=1, device_id={"loc": flip(me, off, n_loc)}, device_id_type=pl.DeviceIdType.MESH
        )

    order = send_order(n_loc)
    early, late, held = order[:2], order[2:-1], order[-1]

    halo_load, left_load, hub_load, nbr_load, cnt_load, w_load, bias_load, slot_load, right_load = [
        pltpu.make_async_copy(source, target, loaded.at[number])
        for number, (source, target) in enumerate((
            (halo_hbm, halo_ref), (feat_hbm.at[:, 0:LANES], feat_ref.at[0]), (hub_hbm, hub_ref), (nbr_hbm, nbr_ref),
            (cnt_hbm, cnt_ref), (w_hbm, w_ref), (bias_hbm, bias_ref), (slot_hbm, slot_ref),
            (feat_hbm.at[:, LANES:], feat_ref.at[1]),
        ))
    ]
    for load in (halo_load, left_load, right_load, w_load, bias_load, hub_load, nbr_load, cnt_load, slot_load):
        load.start()

    def times_weight(x_high, x_low):
        return dot(x_high, wh[...]) + dot(x_low, wh[...]) + dot(x_high, wl[...])

    def whole(ref):
        return jnp.concatenate([ref[0], ref[1]], axis=1)

    def gather(source, peer, target):
        first = peer * listed

        def rows_of(step, carry):
            at = first + step * chunk
            for inner in range(chunk):
                row = halo_ref[at + inner]
                for side in range(2):
                    target[side, step, inner:inner + 1, :] = source[side, pl.ds(row, 1), :]
            return carry

        lax.fori_loop(0, listed // chunk, rows_of, 0)

    def halo_copy(off):
        return pltpu.make_async_remote_copy(
            src_ref=outgoing.at[off],
            dst_ref=recv.at[me],
            send_sem=halo_s.at[off],
            recv_sem=halo_r.at[off],
            device_id={"loc": flip(me, off, n_loc)},
            device_id_type=pl.DeviceIdType.MESH,
        )

    def held_copy(side):
        return pltpu.make_async_remote_copy(
            src_ref=outgoing.at[held, side],
            dst_ref=recv.at[me, side],
            send_sem=halo_s.at[held * (1 - side)],
            recv_sem=halo_r.at[held * (1 - side)],
            device_id={"loc": flip(me, held, n_loc)},
            device_id_type=pl.DeviceIdType.MESH,
        )

    def grp_copy(off):
        target = (grp + off) % n_grp
        return pltpu.make_async_remote_copy(
            src_ref=part.at[pl.ds(pl.multiple_of(target * hub_grp, hub_grp), hub_grp)],
            dst_ref=part_in.at[off],
            send_sem=grp_s.at[off],
            recv_sem=grp_r.at[off],
            device_id={"grp": target},
            device_id_type=pl.DeviceIdType.MESH,
        )

    def loc_copy(off):
        target = flip(me, off, n_loc)
        return pltpu.make_async_remote_copy(
            src_ref=spread.at[target],
            dst_ref=spread_in.at[off],
            send_sem=loc_s.at[off],
            recv_sem=loc_r.at[off],
            device_id={"loc": target},
            device_id_type=pl.DeviceIdType.MESH,
        )

    halo_load.wait()
    left_load.wait()
    right_load.wait()
    for off in early:
        gather(feat_ref, flip(me, off, n_loc), outgoing.at[off])

    @pl.when(me != 1)
    def _():
        pl.semaphore_wait(barrier, n_loc - 1)
        for off in early:
            halo_copy(off).start()

    @pl.when(me == 0)
    def _():
        for off in range(1, n_grp):
            pl.semaphore_signal(
                barrier, inc=1, device_id={"grp": (grp + off) % n_grp, "loc": 1},
                device_id_type=pl.DeviceIdType.MESH,
            )

    w_load.wait()
    w_high, w_low = split(w_ref[...])
    wh[...] = w_high
    wl[...] = w_low
    high, low = split(whole(feat_ref))
    fh[...] = high
    product = times_weight(high, low)
    for side in range(2):
        prod[side] = product[:, side * LANES:(side + 1) * LANES]
    p_high, p_low = split(product)
    ph[...] = p_high
    pl_[...] = p_low

    for off in late + [held]:
        gather(prod, flip(me, off, n_loc), outgoing.at[off])

    def send_late():
        for off in late:
            halo_copy(off).start()
        held_copy(0).start()

    @pl.when(me != 1)
    def _():
        send_late()

    gather(prod, me, recv.at[me])

    hub_load.wait()
    part[...] = dot(hub_ref[...], fh[...])

    nbr_load.wait()
    cnt_load.wait()
    slot = nbr_ref[...]
    used = iota((slots, rows), 0) < jnp.broadcast_to(cnt_ref[...], (slots, rows))
    table[:, 0:slots] = jnp.transpose(jnp.where(used, slot, -1))
    flat = jnp.concatenate(
        [table[pl.ds(vertex, blocks, stride=per_block), 0:slots] for vertex in range(per_block)], axis=1
    )
    level = jnp.where(flat < 0, -1, lax.shift_right_logical(flat, 7))
    codes[...] = level * per_block + iota((blocks, 256), 1) // slots
    lows[...] = flat & (LANES - 1)
    inv[...] = 1.0 / jnp.transpose(jnp.broadcast_to(cnt_ref[...].astype(F32), (LANES, rows)))

    group = 8
    own = rows // 256

    def build(step, carry):
        for inner in range(group):
            block = step * group + inner
            code = codes[pl.ds(block, 1), :]
            spot = lows[pl.ds(block, 1), :]
            left = onehot(iota((levels * per_block, 256), 0) == code)
            right = onehot(iota((LANES, 256), 0) == spot)
            counted = dot_nt(left, right).astype(BF)
            at = pl.ds(pl.multiple_of(block * per_block, per_block), per_block)
            for tile in range(levels):
                piece = counted[tile * per_block:(tile + 1) * per_block]
                if tile < 2 * own:
                    adj_own[at, tile * LANES:(tile + 1) * LANES] = piece
                else:
                    adj[tile - 2 * own, at, :] = piece
        return carry

    steps = blocks // group
    lax.fori_loop(0, steps // 4, build, 0)

    @pl.when(me == 1)
    def _():
        pl.semaphore_wait(barrier, n_loc - 1 + n_grp - 1)
        for off in range(1, n_loc):
            pl.semaphore_signal(
                go, inc=1, device_id={"loc": flip(me, off, n_loc)}, device_id_type=pl.DeviceIdType.MESH
            )
        pl.semaphore_signal(go, inc=1)
        for off in early:
            halo_copy(off).start()
        send_late()

    lax.fori_loop(steps // 4, steps // 2, build, 0)
    pl.semaphore_wait(go, 1)
    for off in range(1, n_grp):
        grp_copy(off).start()
    lax.fori_loop(steps // 2, steps, build, 0)
    acc[...] = dot(adj_own[...], ph[...]) + dot(adj_own[...], pl_[...])

    for off in range(1, n_grp):
        grp_copy(off).wait_recv()
    group_sum = part[pl.ds(pl.multiple_of(grp * hub_grp, hub_grp), hub_grp), :]
    for off in range(1, n_grp):
        group_sum = group_sum + part_in[off]
    if 2 * hub_dev < spread.shape[1]:
        spread[...] = jnp.zeros_like(spread)
    for owner in range(n_loc):
        own_rows = group_sum[owner * hub_dev:(owner + 1) * hub_dev]
        spread[owner, 0:hub_dev, :] = own_rows[:, 0:width // 2]
        spread[owner, hub_dev:2 * hub_dev, :] = own_rows[:, width // 2:]
    for off in range(1, n_loc):
        loc_copy(off).start()
    held_copy(1).start()

    def take(off):
        peer = flip(me, off, n_loc)
        got = jnp.concatenate([recv[peer, side].reshape(listed, LANES) for side in range(2)], axis=1)
        if off in early:
            got = times_weight(*split(got))
        r_high, r_low = split(got)
        column = adj[peer]
        return dot(jnp.concatenate([column, column], axis=1), jnp.concatenate([r_high, r_low], axis=0))

    acc[...] += take(0)
    for off in [1] + early + late[1:]:
        halo_copy(off).wait_recv()
        acc[...] += take(off)

    hubs = spread[me]
    for off in range(1, n_loc):
        loc_copy(off).wait_recv()
        hubs = hubs + spread_in[off]
    hubs = jnp.concatenate([hubs[0:hub_dev], hubs[hub_dev:2 * hub_dev]], axis=1)
    hubs = jnp.concatenate([hubs, jnp.zeros((LANES - hub_dev, width), F32)], axis=0)
    h_high, h_low = split(times_weight(*split(hubs)))
    slot_load.wait()
    bias_load.wait()
    lane = iota((1, LANES), 1)
    target_row = jnp.full((1, LANES), -1, jnp.int32)
    for hub in range(hub_dev):
        target_row = jnp.where(lane == hub, slot_ref[hub], target_row)
    here = onehot(iota((rows, LANES), 0) == target_row)
    hub_rows = dot(here, h_high) + dot(here, h_low)
    scale = inv[...]
    base[...] = acc[...] * jnp.concatenate([scale, scale], axis=1) + (whole(prod) + bias_ref[...] + hub_rows)

    column = adj[flip(me, held, n_loc)]
    column = jnp.concatenate([column, column], axis=1)
    for side in range(2):
        lanes = slice(side * LANES, (side + 1) * LANES)
        held_copy(side).wait_recv()
        r_high, r_low = split(recv[flip(me, held, n_loc), side].reshape(listed, LANES))
        last = dot(column, jnp.concatenate([r_high, r_low], axis=0))
        out_ref[:, lanes] = jnp.maximum(last * inv[...] + base[:, lanes], 0.0)

    for off in order[:-1]:
        halo_copy(off).wait_send()
    for side in range(2):
        held_copy(side).wait_send()
    for off in range(1, n_loc):
        loc_copy(off).wait_send()
    for off in range(1, n_grp):
        grp_copy(off).wait_send()


def solution(mesh):
    n_grp, n_loc = mesh.shape["grp"], mesh.shape["loc"]

    def on_device(features, hub_block, hub_slot, neighbours, counts, halo_send, weight, bias):
        rows, width = features.shape
        slots = neighbours.shape[1]
        listed = halo_send.shape[1]
        chunk = 32
        hubs = hub_block.shape[0]
        blocks = rows // (256 // slots)
        padded = -(-2 * hub_slot.shape[0] // 8) * 8
        vmem = pl.BlockSpec(memory_space=pltpu.VMEM)
        far = pl.BlockSpec(memory_space=pltpu.HBM)
        sem = pltpu.SemaphoreType.DMA
        return pl.pallas_call(
            functools.partial(kernel, n_grp, n_loc),
            out_shape=jax.ShapeDtypeStruct((rows, width), F32),
            in_specs=[far] * 8,
            out_specs=vmem,
            scratch_shapes=[
                pltpu.VMEM((2, rows, LANES), F32),
                pltpu.VMEM(hub_block.shape, BF),
                pltpu.SMEM(hub_slot.shape, jnp.int32),
                pltpu.VMEM((slots, rows), jnp.int32),
                pltpu.VMEM((1, rows), jnp.int32),
                pltpu.SMEM((halo_send.size,), jnp.int32),
                pltpu.VMEM(weight.shape, F32),
                pltpu.VMEM((1, width), F32),
                sem((9,)),
                pltpu.SemaphoreType.REGULAR,
                pltpu.VMEM((rows, width), BF),
                pltpu.VMEM((rows, width), BF),
                pltpu.VMEM((rows, width), BF),
                pltpu.VMEM((2, rows, LANES), F32),
                pltpu.VMEM((rows, LANES), jnp.int32),
                pltpu.VMEM((rows, width), F32),
                pltpu.VMEM((rows, width), F32),
                pltpu.VMEM((rows, rows), BF),
                pltpu.VMEM((n_loc, rows, LANES), BF),
                pltpu.VMEM((blocks, 256), jnp.int32),
                pltpu.VMEM((blocks, 256), jnp.int32),
                pltpu.VMEM((n_loc, 2, listed // chunk, chunk, LANES), F32),
                pltpu.VMEM((n_loc, 2, listed // chunk, chunk, LANES), F32),
                pltpu.VMEM((hubs, width), F32),
                pltpu.VMEM((n_grp, hubs // n_grp, width), F32),
                pltpu.VMEM((n_loc, padded, width // 2), F32),
                pltpu.VMEM((n_loc, padded, width // 2), F32),
                pltpu.VMEM((rows, LANES), F32),
                pltpu.VMEM(weight.shape, BF),
                pltpu.VMEM(weight.shape, BF),
                sem((n_loc,)), sem((n_loc,)), sem((n_grp,)), sem((n_grp,)), sem((n_loc,)), sem((n_loc,)),
            ],
            compiler_params=pltpu.CompilerParams(
                collective_id=0, has_side_effects=True, vmem_limit_bytes=48 * 1024 * 1024
            ),
        )(
            *[
                pltpu.with_memory_space_constraint(array, pltpu.HBM)
                for array in (
                    features, hub_block, hub_slot, neighbours.T, counts.reshape(1, -1), halo_send.reshape(-1), weight,
                    bias.reshape(1, -1),
                )
            ]
        )

    both = ("grp", "loc")
    return jax.shard_map(
        on_device,
        mesh=mesh,
        in_specs=(P(both, None), P(None, both), P(both), P(both, None), P(both), P(both, None), P(), P()),
        out_specs=P(both, None),
        check_vma=False,
    )
```

```python
import functools

import jax
import jax.numpy as jnp
from jax import lax
from jax.experimental import pallas as pl
from jax.experimental.pallas import tpu as pltpu
from jax.sharding import PartitionSpec as P

BF = jnp.bfloat16
F32 = jnp.float32
LANES = 128


def flip(index, mask, count):
    result = index
    bit = 1
    while bit < count:
        if mask & bit:
            result = result + bit * (1 - 2 * ((index // bit) % 2))
        bit *= 2
    return result


def send_order(count):
    near = [off for off in range(2, count) if bin(off >> 1).count("1") == 1]
    far = [off for off in range(2, count) if bin(off >> 1).count("1") > 1]
    near.sort(key=lambda off: (off & 1, off))
    return near[:2] + [1] + near[2:] + far


def dot(a, b):
    return jnp.dot(a, b, preferred_element_type=F32)


def dot_nt(a, b):
    return lax.dot_general(a, b, (((1,), (1,)), ((), ())), preferred_element_type=F32)


def split(x):
    high = x.astype(BF)
    return high, (x - high.astype(F32)).astype(BF)


def onehot(mask):
    return jnp.where(mask, 1.0, 0.0).astype(BF)


def iota(shape, dim):
    return lax.broadcasted_iota(jnp.int32, shape, dim)


def kernel(
    n_grp, n_loc,
    feat_hbm, hub_hbm, slot_hbm, nbr_hbm, cnt_hbm, halo_hbm, w_hbm, bias_hbm,
    out_ref,
    feat_ref, hub_ref, slot_ref, nbr_ref, cnt_ref, halo_ref, w_ref, bias_ref, loaded,
    near, go, fh, ph, pl_, prod, table, base, acc, adj_own, adj, codes, lows, outgoing, recv, part, part_in, spread, spread_in,
    inv, wh, wl,
    halo_s, halo_r, grp_s, grp_r, loc_s, loc_r,
):
    grp = lax.axis_index("grp")
    me = lax.axis_index("loc")
    rows, width = feat_hbm.shape
    chunk = outgoing.shape[3]
    listed = outgoing.shape[2] * chunk
    slots = nbr_ref.shape[0]
    hub_grp = hub_ref.shape[0] // n_grp
    hub_dev = slot_ref.shape[0]
    levels = rows // LANES + n_loc * listed // LANES
    per_block = 256 // slots
    blocks = rows // per_block

    barrier = pltpu.get_barrier_semaphore()
    for off in range(1, n_loc):
        pl.semaphore_signal(
            barrier, inc=1, device_id={"loc": flip(me, off, n_loc)}, device_id_type=pl.DeviceIdType.MESH
        )

    order = send_order(n_loc)
    early, late, held = order[:2], order[2:-1], order[-1]

    halo_load, left_load, hub_load, nbr_load, cnt_load, w_load, bias_load, slot_load, right_load = [
        pltpu.make_async_copy(source, target, loaded.at[number])
        for number, (source, target) in enumerate((
            (halo_hbm, halo_ref), (feat_hbm.at[:, 0:LANES], feat_ref.at[0]), (hub_hbm, hub_ref), (nbr_hbm, nbr_ref),
            (cnt_hbm, cnt_ref), (w_hbm, w_ref), (bias_hbm, bias_ref), (slot_hbm, slot_ref),
            (feat_hbm.at[:, LANES:], feat_ref.at[1]),
        ))
    ]
    for load in (halo_load, left_load, right_load, w_load, nbr_load, cnt_load):
        load.start()

    def times_weight(x_high, x_low):
        return dot(x_high, wh[...]) + dot(x_low, wh[...]) + dot(x_high, wl[...])

    def whole(ref):
        return jnp.concatenate([ref[0], ref[1]], axis=1)

    def gather(source, peer, target):
        first = peer * listed

        def rows_of(step, carry):
            at = first + step * chunk
            for inner in range(chunk):
                row = halo_ref[at + inner]
                for side in range(2):
                    target[side, step, inner:inner + 1, :] = source[side, pl.ds(row, 1), :]
            return carry

        lax.fori_loop(0, listed // chunk, rows_of, 0)

    def halo_copy(off):
        return pltpu.make_async_remote_copy(
            src_ref=outgoing.at[off],
            dst_ref=recv.at[me],
            send_sem=halo_s.at[off],
            recv_sem=halo_r.at[off],
            device_id={"loc": flip(me, off, n_loc)},
            device_id_type=pl.DeviceIdType.MESH,
        )

    def held_copy(side):
        return pltpu.make_async_remote_copy(
            src_ref=outgoing.at[held, side],
            dst_ref=recv.at[me, side],
            send_sem=halo_s.at[held * (1 - side)],
            recv_sem=halo_r.at[held * (1 - side)],
            device_id={"loc": flip(me, held, n_loc)},
            device_id_type=pl.DeviceIdType.MESH,
        )

    def grp_copy(off):
        target = (grp + off) % n_grp
        return pltpu.make_async_remote_copy(
            src_ref=part.at[pl.ds(pl.multiple_of(target * hub_grp, hub_grp), hub_grp)],
            dst_ref=part_in.at[off],
            send_sem=grp_s.at[off],
            recv_sem=grp_r.at[off],
            device_id={"grp": target},
            device_id_type=pl.DeviceIdType.MESH,
        )

    def loc_copy(off):
        target = flip(me, off, n_loc)
        return pltpu.make_async_remote_copy(
            src_ref=spread.at[target],
            dst_ref=spread_in.at[off],
            send_sem=loc_s.at[off],
            recv_sem=loc_r.at[off],
            device_id={"loc": target},
            device_id_type=pl.DeviceIdType.MESH,
        )

    word = n_loc - 1

    @pl.when(me == word - 1)
    def _():
        pl.semaphore_wait(barrier, n_loc - 1)
        pl.semaphore_signal(near, inc=1, device_id={"loc": word}, device_id_type=pl.DeviceIdType.MESH)
        for off in range(1, n_grp):
            pl.semaphore_signal(
                barrier, inc=1, device_id={"grp": (grp + off) % n_grp, "loc": word},
                device_id_type=pl.DeviceIdType.MESH,
            )

    halo_load.wait()
    left_load.wait()
    right_load.wait()
    for off in early:
        gather(feat_ref, flip(me, off, n_loc), outgoing.at[off])

    @pl.when(jnp.logical_and(me > 1, me < word - 1))
    def _():
        pl.semaphore_wait(barrier, n_loc - 1)

    @pl.when(me == word)
    def _():
        pl.semaphore_wait(near, 1)

    def send_early(when):
        @pl.when(when)
        def _():
            for off in early:
                halo_copy(off).start()

    send_early(me > 1)
    for load in (hub_load, bias_load, slot_load):
        load.start()

    w_load.wait()
    w_high, w_low = split(w_ref[...])
    wh[...] = w_high
    wl[...] = w_low
    high, low = split(whole(feat_ref))
    fh[...] = high
    product = times_weight(high, low)
    for side in range(2):
        prod[side] = product[:, side * LANES:(side + 1) * LANES]
    p_high, p_low = split(product)
    ph[...] = p_high
    pl_[...] = p_low

    nbr_load.wait()
    cnt_load.wait()
    slot = nbr_ref[...]
    used = iota((slots, rows), 0) < jnp.broadcast_to(cnt_ref[...], (slots, rows))
    table[:, 0:slots] = jnp.transpose(jnp.where(used, slot, -1))
    flat = jnp.concatenate(
        [table[pl.ds(vertex, blocks, stride=per_block), 0:slots] for vertex in range(per_block)], axis=1
    )
    level = jnp.where(flat < 0, -1, lax.shift_right_logical(flat, 7))
    codes[...] = level * per_block + iota((blocks, 256), 1) // slots
    lows[...] = flat & (LANES - 1)
    inv[...] = 1.0 / jnp.transpose(jnp.broadcast_to(cnt_ref[...].astype(F32), (LANES, rows)))

    @pl.when(me <= 1)
    def _():
        pl.semaphore_wait(barrier, n_loc - 1)

    send_early(me <= 1)

    for off in late:
        gather(prod, flip(me, off, n_loc), outgoing.at[off])
        halo_copy(off).start()
    gather(prod, flip(me, held, n_loc), outgoing.at[held])
    gather(prod, me, recv.at[me])

    @pl.when(me == word)
    def _():
        pl.semaphore_wait(barrier, n_loc - 1 + n_grp - 1)
        for off in range(1, n_loc):
            pl.semaphore_signal(
                go, inc=1, device_id={"loc": flip(me, off, n_loc)}, device_id_type=pl.DeviceIdType.MESH
            )
        pl.semaphore_signal(go, inc=1)

    hub_load.wait()
    part[...] = dot(hub_ref[...], fh[...])

    group = 8
    own = rows // 256

    def build(step, carry):
        for inner in range(group):
            block = step * group + inner
            code = codes[pl.ds(block, 1), :]
            spot = lows[pl.ds(block, 1), :]
            left = onehot(iota((levels * per_block, 256), 0) == code)
            right = onehot(iota((LANES, 256), 0) == spot)
            counted = dot_nt(left, right).astype(BF)
            at = pl.ds(pl.multiple_of(block * per_block, per_block), per_block)
            for tile in range(levels):
                piece = counted[tile * per_block:(tile + 1) * per_block]
                if tile < 2 * own:
                    adj_own[at, tile * LANES:(tile + 1) * LANES] = piece
                else:
                    adj[tile - 2 * own, at, :] = piece
        return carry

    steps = blocks // group
    lax.fori_loop(0, steps // 4, build, 0)
    pl.semaphore_wait(go, 1)
    for off in range(1, n_grp):
        grp_copy(off).start()
    lax.fori_loop(steps // 4, steps, build, 0)
    acc[...] = dot(adj_own[...], ph[...]) + dot(adj_own[...], pl_[...])

    for off in range(1, n_grp):
        grp_copy(off).wait_recv()
    group_sum = part[pl.ds(pl.multiple_of(grp * hub_grp, hub_grp), hub_grp), :]
    for off in range(1, n_grp):
        group_sum = group_sum + part_in[off]
    group_sum = times_weight(*split(group_sum))
    if 2 * hub_dev < spread.shape[1]:
        spread[...] = jnp.zeros_like(spread)
    for owner in range(n_loc):
        own_rows = group_sum[owner * hub_dev:(owner + 1) * hub_dev]
        spread[owner, 0:hub_dev, :] = own_rows[:, 0:width // 2]
        spread[owner, hub_dev:2 * hub_dev, :] = own_rows[:, width // 2:]
    for off in range(1, n_loc):
        loc_copy(off).start()
    for side in range(2):
        held_copy(side).start()

    def take(off):
        peer = flip(me, off, n_loc)
        got = jnp.concatenate([recv[peer, side].reshape(listed, LANES) for side in range(2)], axis=1)
        if off in early:
            got = times_weight(*split(got))
        r_high, r_low = split(got)
        column = adj[peer]
        return dot(jnp.concatenate([column, column], axis=1), jnp.concatenate([r_high, r_low], axis=0))

    slot_load.wait()
    bias_load.wait()
    lane = iota((1, LANES), 1)
    target_row = jnp.full((1, LANES), -1, jnp.int32)
    for hub in range(hub_dev):
        target_row = jnp.where(lane == hub, slot_ref[hub], target_row)
    here = onehot(iota((rows, LANES), 0) == target_row)

    acc[...] += take(0)
    for off in [1] + early + late[1:]:
        halo_copy(off).wait_recv()
        acc[...] += take(off)

    scale = inv[...]
    base[...] = acc[...] * jnp.concatenate([scale, scale], axis=1) + (whole(prod) + bias_ref[...])

    hubs = spread[me]
    for off in range(1, n_loc):
        loc_copy(off).wait_recv()
        hubs = hubs + spread_in[off]
    hubs = jnp.concatenate([hubs[0:hub_dev], hubs[hub_dev:2 * hub_dev]], axis=1)
    hubs = jnp.concatenate([hubs, jnp.zeros((LANES - hub_dev, width), F32)], axis=0)
    base[...] += dot(jnp.concatenate([here, here], axis=1), jnp.concatenate(split(hubs), axis=0))

    column = adj[flip(me, held, n_loc)]
    column = jnp.concatenate([column, column], axis=1)
    for side in range(2):
        lanes = slice(side * LANES, (side + 1) * LANES)
        held_copy(side).wait_recv()
        r_high, r_low = split(recv[flip(me, held, n_loc), side].reshape(listed, LANES))
        last = dot(column, jnp.concatenate([r_high, r_low], axis=0))
        out_ref[:, lanes] = jnp.maximum(last * inv[...] + base[:, lanes], 0.0)

    for off in order[:-1]:
        halo_copy(off).wait_send()
    for side in range(2):
        held_copy(side).wait_send()
    for off in range(1, n_loc):
        loc_copy(off).wait_send()
    for off in range(1, n_grp):
        grp_copy(off).wait_send()


def solution(mesh):
    n_grp, n_loc = mesh.shape["grp"], mesh.shape["loc"]

    def on_device(features, hub_block, hub_slot, neighbours, counts, halo_send, weight, bias):
        rows, width = features.shape
        slots = neighbours.shape[1]
        listed = halo_send.shape[1]
        chunk = 32
        hubs = hub_block.shape[0]
        blocks = rows // (256 // slots)
        padded = -(-2 * hub_slot.shape[0] // 8) * 8
        vmem = pl.BlockSpec(memory_space=pltpu.VMEM)
        far = pl.BlockSpec(memory_space=pltpu.HBM)
        sem = pltpu.SemaphoreType.DMA
        return pl.pallas_call(
            functools.partial(kernel, n_grp, n_loc),
            out_shape=jax.ShapeDtypeStruct((rows, width), F32),
            in_specs=[far] * 8,
            out_specs=vmem,
            scratch_shapes=[
                pltpu.VMEM((2, rows, LANES), F32),
                pltpu.VMEM(hub_block.shape, BF),
                pltpu.SMEM(hub_slot.shape, jnp.int32),
                pltpu.VMEM((slots, rows), jnp.int32),
                pltpu.VMEM((1, rows), jnp.int32),
                pltpu.SMEM((halo_send.size,), jnp.int32),
                pltpu.VMEM(weight.shape, F32),
                pltpu.VMEM((1, width), F32),
                sem((9,)),
                pltpu.SemaphoreType.REGULAR,
                pltpu.SemaphoreType.REGULAR,
                pltpu.VMEM((rows, width), BF),
                pltpu.VMEM((rows, width), BF),
                pltpu.VMEM((rows, width), BF),
                pltpu.VMEM((2, rows, LANES), F32),
                pltpu.VMEM((rows, LANES), jnp.int32),
                pltpu.VMEM((rows, width), F32),
                pltpu.VMEM((rows, width), F32),
                pltpu.VMEM((rows, rows), BF),
                pltpu.VMEM((n_loc, rows, LANES), BF),
                pltpu.VMEM((blocks, 256), jnp.int32),
                pltpu.VMEM((blocks, 256), jnp.int32),
                pltpu.VMEM((n_loc, 2, listed // chunk, chunk, LANES), F32),
                pltpu.VMEM((n_loc, 2, listed // chunk, chunk, LANES), F32),
                pltpu.VMEM((hubs, width), F32),
                pltpu.VMEM((n_grp, hubs // n_grp, width), F32),
                pltpu.VMEM((n_loc, padded, width // 2), F32),
                pltpu.VMEM((n_loc, padded, width // 2), F32),
                pltpu.VMEM((rows, LANES), F32),
                pltpu.VMEM(weight.shape, BF),
                pltpu.VMEM(weight.shape, BF),
                sem((n_loc,)), sem((n_loc,)), sem((n_grp,)), sem((n_grp,)), sem((n_loc,)), sem((n_loc,)),
            ],
            compiler_params=pltpu.CompilerParams(
                collective_id=0, has_side_effects=True, vmem_limit_bytes=48 * 1024 * 1024
            ),
        )(
            *[
                pltpu.with_memory_space_constraint(array, pltpu.HBM)
                for array in (
                    features, hub_block, hub_slot, neighbours.T, counts.reshape(1, -1), halo_send.reshape(-1), weight,
                    bias.reshape(1, -1),
                )
            ]
        )

    both = ("grp", "loc")
    return jax.shard_map(
        on_device,
        mesh=mesh,
        in_specs=(P(both, None), P(None, both), P(both), P(both, None), P(both), P(both, None), P(), P()),
        out_specs=P(both, None),
        check_vma=False,
    )
```

```python
import functools

import jax
import jax.numpy as jnp
from jax import lax
from jax.experimental import pallas as pl
from jax.experimental.pallas import tpu as pltpu
from jax.sharding import PartitionSpec as P

BF = jnp.bfloat16
F32 = jnp.float32
LANES = 128


def flip(index, mask, count):
    result = index
    bit = 1
    while bit < count:
        if mask & bit:
            result = result + bit * (1 - 2 * ((index // bit) % 2))
        bit *= 2
    return result


def send_order(count):
    near = [off for off in range(2, count) if bin(off >> 1).count("1") == 1]
    far = [off for off in range(2, count) if bin(off >> 1).count("1") > 1]
    near.sort(key=lambda off: (off & 1, off))
    return near[:2] + [1] + near[2:] + far


def dot(a, b):
    return jnp.dot(a, b, preferred_element_type=F32)


def dot_nt(a, b):
    return lax.dot_general(a, b, (((1,), (1,)), ((), ())), preferred_element_type=F32)


def split(x):
    high = x.astype(BF)
    return high, (x - high.astype(F32)).astype(BF)


def onehot(mask):
    return jnp.where(mask, 1.0, 0.0).astype(BF)


def iota(shape, dim):
    return lax.broadcasted_iota(jnp.int32, shape, dim)


def kernel(
    n_grp, n_loc,
    feat_hbm, hub_hbm, slot_hbm, nbr_hbm, cnt_hbm, halo_hbm, w_hbm, bias_hbm,
    out_ref,
    feat_ref, hub_ref, slot_ref, nbr_ref, cnt_ref, halo_ref, w_ref, bias_ref, loaded,
    near, go, fh, ph, pl_, prod, table, base, acc, adj_own, adj, codes, lows, outgoing, recv, part, part_in, spread, spread_in,
    inv, wh, wl,
    halo_s, halo_r, grp_s, grp_r, loc_s, loc_r,
):
    grp = lax.axis_index("grp")
    me = lax.axis_index("loc")
    rows, width = feat_hbm.shape
    chunk = outgoing.shape[3]
    listed = outgoing.shape[2] * chunk
    slots = nbr_ref.shape[0]
    hub_grp = hub_ref.shape[0] // n_grp
    hub_dev = slot_ref.shape[0]
    levels = rows // LANES + n_loc * listed // LANES
    per_block = 256 // slots
    blocks = rows // per_block

    def all_of(ref, count, send_sem, recv_sem):
        return pltpu.make_async_remote_copy(
            src_ref=ref.at[0:count], dst_ref=ref.at[0:count], send_sem=send_sem, recv_sem=recv_sem,
            device_id={"loc": flip(me, 1, n_loc)}, device_id_type=pl.DeviceIdType.MESH,
        )

    order = send_order(n_loc)
    early, late, held = order[:2], order[2:-1], order[-1]

    halo_load, left_load, hub_load, nbr_load, cnt_load, w_load, bias_load, slot_load, right_load = [
        pltpu.make_async_copy(source, target, loaded.at[number])
        for number, (source, target) in enumerate((
            (halo_hbm, halo_ref), (feat_hbm.at[:, 0:LANES], feat_ref.at[0]), (hub_hbm, hub_ref), (nbr_hbm, nbr_ref),
            (cnt_hbm, cnt_ref), (w_hbm, w_ref), (bias_hbm, bias_ref), (slot_hbm, slot_ref),
            (feat_hbm.at[:, LANES:], feat_ref.at[1]),
        ))
    ]
    for load in (halo_load, left_load, right_load, w_load, nbr_load, cnt_load):
        load.start()

    barrier = pltpu.get_barrier_semaphore()
    for off in range(1, n_loc):
        pl.semaphore_signal(
            barrier, inc=1, device_id={"loc": flip(me, off, n_loc)}, device_id_type=pl.DeviceIdType.MESH
        )


    def times_weight(x_high, x_low):
        return dot(x_high, wh[...]) + dot(x_low, wh[...]) + dot(x_high, wl[...])

    def whole(ref):
        return jnp.concatenate([ref[0], ref[1]], axis=1)

    def gather(source, peer, target):
        first = peer * listed

        def rows_of(step, carry):
            at = first + step * chunk
            for inner in range(chunk):
                row = halo_ref[at + inner]
                for side in range(2):
                    target[side, step, inner:inner + 1, :] = source[side, pl.ds(row, 1), :]
            return carry

        lax.fori_loop(0, listed // chunk, rows_of, 0)

    def halo_copy(off):
        return pltpu.make_async_remote_copy(
            src_ref=outgoing.at[off],
            dst_ref=recv.at[me],
            send_sem=halo_s.at[off],
            recv_sem=halo_r.at[off],
            device_id={"loc": flip(me, off, n_loc)},
            device_id_type=pl.DeviceIdType.MESH,
        )

    def held_copy(side):
        return pltpu.make_async_remote_copy(
            src_ref=outgoing.at[held, side],
            dst_ref=recv.at[me, side],
            send_sem=halo_s.at[held * (1 - side)],
            recv_sem=halo_r.at[held * (1 - side)],
            device_id={"loc": flip(me, held, n_loc)},
            device_id_type=pl.DeviceIdType.MESH,
        )

    def grp_copy(off):
        target = (grp + off) % n_grp
        return pltpu.make_async_remote_copy(
            src_ref=part.at[pl.ds(pl.multiple_of(target * hub_grp, hub_grp), hub_grp)],
            dst_ref=part_in.at[off],
            send_sem=grp_s,
            recv_sem=grp_r,
            device_id={"grp": target},
            device_id_type=pl.DeviceIdType.MESH,
        )

    def loc_copy(off):
        target = flip(me, off, n_loc)
        return pltpu.make_async_remote_copy(
            src_ref=spread.at[target],
            dst_ref=spread_in.at[off],
            send_sem=loc_s,
            recv_sem=loc_r,
            device_id={"loc": target},
            device_id_type=pl.DeviceIdType.MESH,
        )

    word = n_loc - 1

    @pl.when(me == word - 1)
    def _():
        pl.semaphore_wait(barrier, n_loc - 1)
        pl.semaphore_signal(near, inc=1, device_id={"loc": word}, device_id_type=pl.DeviceIdType.MESH)
        for off in range(1, n_grp):
            pl.semaphore_signal(
                barrier, inc=1, device_id={"grp": (grp + off) % n_grp, "loc": word},
                device_id_type=pl.DeviceIdType.MESH,
            )

    halo_load.wait()
    left_load.wait()
    right_load.wait()
    first, second = early
    gather(feat_ref, flip(me, first, n_loc), outgoing.at[first])

    @pl.when(jnp.logical_and(me > 1, me < word - 1))
    def _():
        pl.semaphore_wait(barrier, n_loc - 1)

    @pl.when(me == word)
    def _():
        pl.semaphore_wait(near, 1)

    def send_early(off, when):
        @pl.when(when)
        def _():
            halo_copy(off).start()

    send_early(first, me > 1)
    gather(feat_ref, flip(me, second, n_loc), outgoing.at[second])
    send_early(second, me > 1)
    for load in (hub_load, bias_load, slot_load):
        load.start()

    w_load.wait()
    w_high, w_low = split(w_ref[...])
    wh[...] = w_high
    wl[...] = w_low
    high, low = split(whole(feat_ref))
    fh[...] = high
    product = times_weight(high, low)
    for side in range(2):
        prod[side] = product[:, side * LANES:(side + 1) * LANES]
    p_high, p_low = split(product)
    ph[...] = p_high
    pl_[...] = p_low

    @pl.when(me <= 1)
    def _():
        pl.semaphore_wait(barrier, n_loc - 1)

    for off in early:
        send_early(off, me <= 1)

    nbr_load.wait()
    cnt_load.wait()
    slot = nbr_ref[...]
    used = iota((slots, rows), 0) < jnp.broadcast_to(cnt_ref[...], (slots, rows))
    table[:, 0:slots] = jnp.transpose(jnp.where(used, slot, -1))
    flat = jnp.concatenate(
        [table[pl.ds(vertex, blocks, stride=per_block), 0:slots] for vertex in range(per_block)], axis=1
    )
    level = jnp.where(flat < 0, -1, lax.shift_right_logical(flat, 7))
    codes[...] = level * per_block + iota((blocks, 256), 1) // slots
    lows[...] = flat & (LANES - 1)
    inv[...] = 1.0 / jnp.transpose(jnp.broadcast_to(cnt_ref[...].astype(F32), (LANES, rows)))

    for off in late:
        gather(prod, flip(me, off, n_loc), outgoing.at[off])
        halo_copy(off).start()
    gather(prod, flip(me, held, n_loc), outgoing.at[held])
    gather(prod, me, recv.at[me])

    @pl.when(me == word)
    def _():
        pl.semaphore_wait(barrier, n_loc - 1 + n_grp - 1)
        for off in range(1, n_loc):
            pl.semaphore_signal(
                go, inc=1, device_id={"loc": flip(me, off, n_loc)}, device_id_type=pl.DeviceIdType.MESH
            )
        pl.semaphore_signal(go, inc=1)

    hub_load.wait()
    part[...] = dot(hub_ref[...], fh[...])

    group = 8
    own = rows // 256

    def build(step, carry):
        for inner in range(group):
            block = step * group + inner
            code = codes[pl.ds(block, 1), :]
            spot = lows[pl.ds(block, 1), :]
            left = onehot(iota((levels * per_block, 256), 0) == code)
            right = onehot(iota((LANES, 256), 0) == spot)
            counted = dot_nt(left, right).astype(BF)
            at = pl.ds(pl.multiple_of(block * per_block, per_block), per_block)
            for tile in range(levels):
                piece = counted[tile * per_block:(tile + 1) * per_block]
                if tile < 2 * own:
                    adj_own[at, tile * LANES:(tile + 1) * LANES] = piece
                else:
                    adj[tile - 2 * own, at, :] = piece
        return carry

    steps = blocks // group
    lax.fori_loop(0, steps // 4, build, 0)
    pl.semaphore_wait(go, 1)
    for off in range(1, n_grp):
        grp_copy(off).start()
    lax.fori_loop(steps // 4, steps, build, 0)
    acc[...] = dot(adj_own[...], ph[...]) + dot(adj_own[...], pl_[...])

    all_of(part_in, n_grp - 1, grp_s, grp_r).wait_recv()
    group_sum = part[pl.ds(pl.multiple_of(grp * hub_grp, hub_grp), hub_grp), :]
    for off in range(1, n_grp):
        group_sum = group_sum + part_in[off]
    group_sum = times_weight(*split(group_sum))
    if 2 * hub_dev < spread.shape[1]:
        spread[...] = jnp.zeros_like(spread)
    for owner in range(n_loc):
        own_rows = group_sum[owner * hub_dev:(owner + 1) * hub_dev]
        spread[owner, 0:hub_dev, :] = own_rows[:, 0:width // 2]
        spread[owner, hub_dev:2 * hub_dev, :] = own_rows[:, width // 2:]
    for off in range(1, n_loc):
        loc_copy(off).start()
    for side in range(2):
        held_copy(side).start()

    def take(off):
        peer = flip(me, off, n_loc)
        got = jnp.concatenate([recv[peer, side].reshape(listed, LANES) for side in range(2)], axis=1)
        if off in early:
            got = times_weight(*split(got))
        r_high, r_low = split(got)
        column = adj[peer]
        return dot(jnp.concatenate([column, column], axis=1), jnp.concatenate([r_high, r_low], axis=0))

    slot_load.wait()
    bias_load.wait()
    lane = iota((1, LANES), 1)
    target_row = jnp.full((1, LANES), -1, jnp.int32)
    for hub in range(hub_dev):
        target_row = jnp.where(lane == hub, slot_ref[hub], target_row)
    here = onehot(iota((rows, LANES), 0) == target_row)

    acc[...] += take(0)
    for off in [1] + early + late[1:]:
        halo_copy(off).wait_recv()
        acc[...] += take(off)

    scale = inv[...]
    base[...] = acc[...] * jnp.concatenate([scale, scale], axis=1) + (whole(prod) + bias_ref[...])

    hubs = spread[me]
    all_of(spread_in, n_loc - 1, loc_s, loc_r).wait_recv()
    for off in range(1, n_loc):
        hubs = hubs + spread_in[off]
    hubs = jnp.concatenate([hubs[0:hub_dev], hubs[hub_dev:2 * hub_dev]], axis=1)
    hubs = jnp.concatenate([hubs, jnp.zeros((LANES - hub_dev, width), F32)], axis=0)
    base[...] += dot(jnp.concatenate([here, here], axis=1), jnp.concatenate(split(hubs), axis=0))

    peer = flip(me, held, n_loc)
    parts = [slice(part * rows // 2, (part + 1) * rows // 2) for part in range(2)]
    for side in range(2):
        lanes = slice(side * LANES, (side + 1) * LANES)
        held_copy(side).wait_recv()
        pair = jnp.concatenate(split(recv[peer, side].reshape(listed, LANES)), axis=0)
        for at in parts:
            column = adj[peer, at, :]
            last = dot(jnp.concatenate([column, column], axis=1), pair)
            out_ref[at, lanes] = jnp.maximum(last * inv[at, :] + base[at, lanes], 0.0)

    for off in order[:-1]:
        halo_copy(off).wait_send()
    for side in range(2):
        held_copy(side).wait_send()
    all_of(spread_in, n_loc - 1, loc_s, loc_r).wait_send()
    all_of(part_in, n_grp - 1, grp_s, grp_r).wait_send()


def solution(mesh):
    n_grp, n_loc = mesh.shape["grp"], mesh.shape["loc"]

    def on_device(features, hub_block, hub_slot, neighbours, counts, halo_send, weight, bias):
        rows, width = features.shape
        slots = neighbours.shape[1]
        listed = halo_send.shape[1]
        chunk = 32
        hubs = hub_block.shape[0]
        blocks = rows // (256 // slots)
        padded = -(-2 * hub_slot.shape[0] // 8) * 8
        vmem = pl.BlockSpec(memory_space=pltpu.VMEM)
        far = pl.BlockSpec(memory_space=pltpu.HBM)
        sem = pltpu.SemaphoreType.DMA
        return pl.pallas_call(
            functools.partial(kernel, n_grp, n_loc),
            out_shape=jax.ShapeDtypeStruct((rows, width), F32),
            in_specs=[far] * 8,
            out_specs=vmem,
            scratch_shapes=[
                pltpu.VMEM((2, rows, LANES), F32),
                pltpu.VMEM(hub_block.shape, BF),
                pltpu.SMEM(hub_slot.shape, jnp.int32),
                pltpu.VMEM((slots, rows), jnp.int32),
                pltpu.VMEM((1, rows), jnp.int32),
                pltpu.SMEM((halo_send.size,), jnp.int32),
                pltpu.VMEM(weight.shape, F32),
                pltpu.VMEM((1, width), F32),
                sem((9,)),
                pltpu.SemaphoreType.REGULAR,
                pltpu.SemaphoreType.REGULAR,
                pltpu.VMEM((rows, width), BF),
                pltpu.VMEM((rows, width), BF),
                pltpu.VMEM((rows, width), BF),
                pltpu.VMEM((2, rows, LANES), F32),
                pltpu.VMEM((rows, LANES), jnp.int32),
                pltpu.VMEM((rows, width), F32),
                pltpu.VMEM((rows, width), F32),
                pltpu.VMEM((rows, rows), BF),
                pltpu.VMEM((n_loc, rows, LANES), BF),
                pltpu.VMEM((blocks, 256), jnp.int32),
                pltpu.VMEM((blocks, 256), jnp.int32),
                pltpu.VMEM((n_loc, 2, listed // chunk, chunk, LANES), F32),
                pltpu.VMEM((n_loc, 2, listed // chunk, chunk, LANES), F32),
                pltpu.VMEM((hubs, width), F32),
                pltpu.VMEM((n_grp, hubs // n_grp, width), F32),
                pltpu.VMEM((n_loc, padded, width // 2), F32),
                pltpu.VMEM((n_loc, padded, width // 2), F32),
                pltpu.VMEM((rows, LANES), F32),
                pltpu.VMEM(weight.shape, BF),
                pltpu.VMEM(weight.shape, BF),
                sem((n_loc,)), sem((n_loc,)), sem, sem, sem, sem,
            ],
            compiler_params=pltpu.CompilerParams(
                collective_id=0, has_side_effects=True, vmem_limit_bytes=48 * 1024 * 1024
            ),
        )(
            *[
                pltpu.with_memory_space_constraint(array, pltpu.HBM)
                for array in (
                    features, hub_block, hub_slot, neighbours.T, counts.reshape(1, -1), halo_send.reshape(-1), weight,
                    bias.reshape(1, -1),
                )
            ]
        )

    both = ("grp", "loc")
    return jax.shard_map(
        on_device,
        mesh=mesh,
        in_specs=(P(both, None), P(None, both), P(both), P(both, None), P(both), P(both, None), P(), P()),
        out_specs=P(both, None),
        check_vma=False,
    )
```

```python
import functools

import jax
import jax.numpy as jnp
from jax import lax
from jax.experimental import pallas as pl
from jax.experimental.pallas import tpu as pltpu
from jax.sharding import PartitionSpec as P

BF = jnp.bfloat16
F32 = jnp.float32
LANES = 128


def flip(index, mask, count):
    result = index
    bit = 1
    while bit < count:
        if mask & bit:
            result = result + bit * (1 - 2 * ((index // bit) % 2))
        bit *= 2
    return result


def send_order(count):
    near = [off for off in range(2, count) if bin(off >> 1).count("1") == 1]
    far = [off for off in range(2, count) if bin(off >> 1).count("1") > 1]
    near.sort(key=lambda off: (off & 1, off))
    return near[:2] + [1] + near[2:] + far


def dot(a, b):
    return jnp.dot(a, b, preferred_element_type=F32)


def dot_nt(a, b):
    return lax.dot_general(a, b, (((1,), (1,)), ((), ())), preferred_element_type=F32)


def split(x):
    high = x.astype(BF)
    return high, (x - high.astype(F32)).astype(BF)


def onehot(mask):
    return jnp.where(mask, 1.0, 0.0).astype(BF)


def iota(shape, dim):
    return lax.broadcasted_iota(jnp.int32, shape, dim)


def kernel(
    n_grp, n_loc,
    feat_hbm, hub_hbm, slot_hbm, nbr_hbm, cnt_hbm, halo_hbm, w_hbm, bias_hbm,
    out_ref,
    feat_ref, hub_ref, slot_ref, nbr_ref, cnt_ref, halo_ref, w_ref, bias_ref, loaded,
    near, go, fh, ph, pl_, prod, table, base, acc, adj_own, adj, codes, lows, outgoing, recv, mine, pair_in, part, part_in, spread, spread_in,
    inv, wh, wl,
    halo_s, halo_r, pair_s, pair_r, grp_s, grp_r, loc_s, loc_r,
):
    grp = lax.axis_index("grp")
    me = lax.axis_index("loc")
    rows, width = feat_hbm.shape
    chunk = outgoing.shape[3]
    listed = outgoing.shape[2] * chunk
    slots = nbr_ref.shape[0]
    hub_dev = slot_ref.shape[0]
    levels = rows // LANES + n_loc * listed // LANES
    per_block = 256 // slots
    blocks = rows // per_block

    def all_of(ref, count, send_sem, recv_sem):
        return pltpu.make_async_remote_copy(
            src_ref=ref.at[0:count], dst_ref=ref.at[0:count], send_sem=send_sem, recv_sem=recv_sem,
            device_id={"loc": flip(me, 1, n_loc)}, device_id_type=pl.DeviceIdType.MESH,
        )

    order = send_order(n_loc)
    early, late, held = order[:2], order[2:-1], order[-1]

    halo_load, left_load, hub_load, nbr_load, cnt_load, w_load, bias_load, slot_load, right_load = [
        pltpu.make_async_copy(source, target, loaded.at[number])
        for number, (source, target) in enumerate((
            (halo_hbm, halo_ref), (feat_hbm.at[:, 0:LANES], feat_ref.at[0]), (hub_hbm, hub_ref), (nbr_hbm, nbr_ref),
            (cnt_hbm, cnt_ref), (w_hbm, w_ref), (bias_hbm, bias_ref), (slot_hbm, slot_ref),
            (feat_hbm.at[:, LANES:], feat_ref.at[1]),
        ))
    ]
    for load in (halo_load, left_load, right_load, w_load, nbr_load, cnt_load):
        load.start()

    barrier = pltpu.get_barrier_semaphore()
    for off in range(1, n_loc):
        pl.semaphore_signal(
            barrier, inc=1, device_id={"loc": flip(me, off, n_loc)}, device_id_type=pl.DeviceIdType.MESH
        )


    def times_weight(x_high, x_low):
        return dot(x_high, wh[...]) + dot(x_low, wh[...]) + dot(x_high, wl[...])

    def whole(ref):
        return jnp.concatenate([ref[0], ref[1]], axis=1)

    def gather(source, peer, target):
        first = peer * listed

        def rows_of(step, carry):
            at = first + step * chunk
            for inner in range(chunk):
                row = halo_ref[at + inner]
                for side in range(2):
                    target[side, step, inner:inner + 1, :] = source[side, pl.ds(row, 1), :]
            return carry

        lax.fori_loop(0, listed // chunk, rows_of, 0)

    def halo_copy(off):
        return pltpu.make_async_remote_copy(
            src_ref=outgoing.at[off],
            dst_ref=recv.at[me],
            send_sem=halo_s.at[off],
            recv_sem=halo_r.at[off],
            device_id={"loc": flip(me, off, n_loc)},
            device_id_type=pl.DeviceIdType.MESH,
        )

    def held_copy(side):
        return pltpu.make_async_remote_copy(
            src_ref=outgoing.at[held, side],
            dst_ref=recv.at[me, side],
            send_sem=halo_s.at[held * (1 - side)],
            recv_sem=halo_r.at[held * (1 - side)],
            device_id={"loc": flip(me, held, n_loc)},
            device_id_type=pl.DeviceIdType.MESH,
        )

    core = me % 2
    pair_copy = pltpu.make_async_remote_copy(
        src_ref=mine.at[1 - core], dst_ref=pair_in, send_sem=pair_s, recv_sem=pair_r,
        device_id={"loc": flip(me, 1, n_loc)}, device_id_type=pl.DeviceIdType.MESH,
    )

    def grp_copy(off):
        target = (grp + off) % n_grp
        return pltpu.make_async_remote_copy(
            src_ref=part.at[target],
            dst_ref=part_in.at[off],
            send_sem=grp_s,
            recv_sem=grp_r,
            device_id={"grp": target},
            device_id_type=pl.DeviceIdType.MESH,
        )

    def loc_copy(off):
        target = flip(me, off, n_loc)
        return pltpu.make_async_remote_copy(
            src_ref=spread.at[target // 2],
            dst_ref=spread_in.at[off // 2],
            send_sem=loc_s,
            recv_sem=loc_r,
            device_id={"loc": target},
            device_id_type=pl.DeviceIdType.MESH,
        )

    word = n_loc - 1

    @pl.when(me == word - 1)
    def _():
        pl.semaphore_wait(barrier, n_loc - 1)
        pl.semaphore_signal(near, inc=1, device_id={"loc": word}, device_id_type=pl.DeviceIdType.MESH)
        for off in range(1, n_grp):
            pl.semaphore_signal(
                barrier, inc=1, device_id={"grp": (grp + off) % n_grp, "loc": word},
                device_id_type=pl.DeviceIdType.MESH,
            )

    halo_load.wait()
    left_load.wait()
    right_load.wait()
    first, second = early
    gather(feat_ref, flip(me, first, n_loc), outgoing.at[first])

    @pl.when(jnp.logical_and(me > 1, me < word - 1))
    def _():
        pl.semaphore_wait(barrier, n_loc - 1)

    @pl.when(me == word)
    def _():
        pl.semaphore_wait(near, 1)

    def send_early(off, when):
        @pl.when(when)
        def _():
            halo_copy(off).start()

    send_early(first, me > 1)
    gather(feat_ref, flip(me, second, n_loc), outgoing.at[second])
    send_early(second, me > 1)
    for load in (hub_load, bias_load, slot_load):
        load.start()

    w_load.wait()
    w_high, w_low = split(w_ref[...])
    wh[...] = w_high
    wl[...] = w_low
    high, low = split(whole(feat_ref))
    fh[...] = high
    product = times_weight(high, low)
    for side in range(2):
        prod[side] = product[:, side * LANES:(side + 1) * LANES]
    p_high, p_low = split(product)
    ph[...] = p_high
    pl_[...] = p_low

    @pl.when(me <= 1)
    def _():
        pl.semaphore_wait(barrier, n_loc - 1)

    for off in early:
        send_early(off, me <= 1)

    nbr_load.wait()
    cnt_load.wait()
    slot = nbr_ref[...]
    used = iota((slots, rows), 0) < jnp.broadcast_to(cnt_ref[...], (slots, rows))
    table[:, 0:slots] = jnp.transpose(jnp.where(used, slot, -1))
    flat = jnp.concatenate(
        [table[pl.ds(vertex, blocks, stride=per_block), 0:slots] for vertex in range(per_block)], axis=1
    )
    level = jnp.where(flat < 0, -1, lax.shift_right_logical(flat, 7))
    codes[...] = level * per_block + iota((blocks, 256), 1) // slots
    lows[...] = flat & (LANES - 1)
    inv[...] = 1.0 / jnp.transpose(jnp.broadcast_to(cnt_ref[...].astype(F32), (LANES, rows)))

    for off in late:
        gather(prod, flip(me, off, n_loc), outgoing.at[off])
        halo_copy(off).start()
    gather(prod, flip(me, held, n_loc), outgoing.at[held])
    gather(prod, me, recv.at[me])

    hub_load.wait()
    product = dot(hub_ref[...], fh[...])
    for side in range(2):
        mine[side] = jnp.concatenate(
            [product[owner * hub_dev:(owner + 1) * hub_dev] for owner in range(side, n_grp * n_loc, 2)], axis=0
        )
    pair_copy.start()

    @pl.when(me == word)
    def _():
        pl.semaphore_wait(barrier, n_loc - 1 + n_grp - 1)
        for off in range(1, n_loc):
            pl.semaphore_signal(
                go, inc=1, device_id={"loc": flip(me, off, n_loc)}, device_id_type=pl.DeviceIdType.MESH
            )
        pl.semaphore_signal(go, inc=1)


    group = 8
    own = rows // 256

    def build(step, carry):
        for inner in range(group):
            block = step * group + inner
            code = codes[pl.ds(block, 1), :]
            spot = lows[pl.ds(block, 1), :]
            left = onehot(iota((levels * per_block, 256), 0) == code)
            right = onehot(iota((LANES, 256), 0) == spot)
            counted = dot_nt(left, right).astype(BF)
            at = pl.ds(pl.multiple_of(block * per_block, per_block), per_block)
            for tile in range(levels):
                piece = counted[tile * per_block:(tile + 1) * per_block]
                if tile < 2 * own:
                    adj_own[at, tile * LANES:(tile + 1) * LANES] = piece
                else:
                    adj[tile - 2 * own, at, :] = piece
        return carry

    steps = blocks // group
    lax.fori_loop(0, steps // 4, build, 0)
    pair_copy.wait_recv()
    part[...] = (mine[core] + pair_in[...]).reshape(part.shape)
    pl.semaphore_wait(go, 1)
    for off in range(1, n_grp):
        grp_copy(off).start()
    lax.fori_loop(steps // 4, steps, build, 0)
    acc[...] = dot(adj_own[...], ph[...]) + dot(adj_own[...], pl_[...])

    all_of(part_in, n_grp - 1, grp_s, grp_r).wait_recv()
    group_sum = part[grp]
    for off in range(1, n_grp):
        group_sum = group_sum + part_in[off]
    group_sum = times_weight(*split(group_sum))
    if 2 * hub_dev < spread.shape[1]:
        spread[...] = jnp.zeros_like(spread)
    for owner in range(n_loc // 2):
        own_rows = group_sum[owner * hub_dev:(owner + 1) * hub_dev]
        spread[owner, 0:hub_dev, :] = own_rows[:, 0:width // 2]
        spread[owner, hub_dev:2 * hub_dev, :] = own_rows[:, width // 2:]
    for off in range(2, n_loc, 2):
        loc_copy(off).start()
    for side in range(2):
        held_copy(side).start()

    def take(off):
        peer = flip(me, off, n_loc)
        got = jnp.concatenate([recv[peer, side].reshape(listed, LANES) for side in range(2)], axis=1)
        if off in early:
            got = times_weight(*split(got))
        r_high, r_low = split(got)
        column = adj[peer]
        return dot(jnp.concatenate([column, column], axis=1), jnp.concatenate([r_high, r_low], axis=0))

    slot_load.wait()
    bias_load.wait()
    lane = iota((1, LANES), 1)
    target_row = jnp.full((1, LANES), -1, jnp.int32)
    for hub in range(hub_dev):
        target_row = jnp.where(lane == hub, slot_ref[hub], target_row)
    here = onehot(iota((rows, LANES), 0) == target_row)

    acc[...] += take(0)
    for off in [1] + early + late[1:]:
        halo_copy(off).wait_recv()
        acc[...] += take(off)

    scale = inv[...]
    base[...] = acc[...] * jnp.concatenate([scale, scale], axis=1) + (whole(prod) + bias_ref[...])

    hubs = spread[me // 2]
    all_of(spread_in, n_loc // 2 - 1, loc_s, loc_r).wait_recv()
    for off in range(2, n_loc, 2):
        hubs = hubs + spread_in[off // 2]
    hubs = jnp.concatenate([hubs[0:hub_dev], hubs[hub_dev:2 * hub_dev]], axis=1)
    hubs = jnp.concatenate([hubs, jnp.zeros((LANES - hub_dev, width), F32)], axis=0)
    base[...] += dot(jnp.concatenate([here, here], axis=1), jnp.concatenate(split(hubs), axis=0))

    peer = flip(me, held, n_loc)
    parts = [slice(part * rows // 2, (part + 1) * rows // 2) for part in range(2)]
    for side in range(2):
        lanes = slice(side * LANES, (side + 1) * LANES)
        held_copy(side).wait_recv()
        pair = jnp.concatenate(split(recv[peer, side].reshape(listed, LANES)), axis=0)
        for at in parts:
            column = adj[peer, at, :]
            last = dot(jnp.concatenate([column, column], axis=1), pair)
            out_ref[at, lanes] = jnp.maximum(last * inv[at, :] + base[at, lanes], 0.0)

    for off in order[:-1]:
        halo_copy(off).wait_send()
    for side in range(2):
        held_copy(side).wait_send()
    all_of(spread_in, n_loc // 2 - 1, loc_s, loc_r).wait_send()
    pair_copy.wait_send()
    all_of(part_in, n_grp - 1, grp_s, grp_r).wait_send()


def solution(mesh):
    n_grp, n_loc = mesh.shape["grp"], mesh.shape["loc"]

    def on_device(features, hub_block, hub_slot, neighbours, counts, halo_send, weight, bias):
        rows, width = features.shape
        slots = neighbours.shape[1]
        listed = halo_send.shape[1]
        chunk = 32
        hubs = hub_block.shape[0]
        blocks = rows // (256 // slots)
        padded = -(-2 * hub_slot.shape[0] // 8) * 8
        vmem = pl.BlockSpec(memory_space=pltpu.VMEM)
        far = pl.BlockSpec(memory_space=pltpu.HBM)
        sem = pltpu.SemaphoreType.DMA
        return pl.pallas_call(
            functools.partial(kernel, n_grp, n_loc),
            out_shape=jax.ShapeDtypeStruct((rows, width), F32),
            in_specs=[far] * 8,
            out_specs=vmem,
            scratch_shapes=[
                pltpu.VMEM((2, rows, LANES), F32),
                pltpu.VMEM(hub_block.shape, BF),
                pltpu.SMEM(hub_slot.shape, jnp.int32),
                pltpu.VMEM((slots, rows), jnp.int32),
                pltpu.VMEM((1, rows), jnp.int32),
                pltpu.SMEM((halo_send.size,), jnp.int32),
                pltpu.VMEM(weight.shape, F32),
                pltpu.VMEM((1, width), F32),
                sem((9,)),
                pltpu.SemaphoreType.REGULAR,
                pltpu.SemaphoreType.REGULAR,
                pltpu.VMEM((rows, width), BF),
                pltpu.VMEM((rows, width), BF),
                pltpu.VMEM((rows, width), BF),
                pltpu.VMEM((2, rows, LANES), F32),
                pltpu.VMEM((rows, LANES), jnp.int32),
                pltpu.VMEM((rows, width), F32),
                pltpu.VMEM((rows, width), F32),
                pltpu.VMEM((rows, rows), BF),
                pltpu.VMEM((n_loc, rows, LANES), BF),
                pltpu.VMEM((blocks, 256), jnp.int32),
                pltpu.VMEM((blocks, 256), jnp.int32),
                pltpu.VMEM((n_loc, 2, listed // chunk, chunk, LANES), F32),
                pltpu.VMEM((n_loc, 2, listed // chunk, chunk, LANES), F32),
                pltpu.VMEM((2, hubs // 2, width), F32),
                pltpu.VMEM((hubs // 2, width), F32),
                pltpu.VMEM((n_grp, hubs // n_grp // 2, width), F32),
                pltpu.VMEM((n_grp, hubs // n_grp // 2, width), F32),
                pltpu.VMEM((n_loc // 2, padded, width // 2), F32),
                pltpu.VMEM((n_loc // 2, padded, width // 2), F32),
                pltpu.VMEM((rows, LANES), F32),
                pltpu.VMEM(weight.shape, BF),
                pltpu.VMEM(weight.shape, BF),
                sem((n_loc,)), sem((n_loc,)), sem, sem, sem, sem, sem, sem,
            ],
            compiler_params=pltpu.CompilerParams(
                collective_id=0, has_side_effects=True, vmem_limit_bytes=48 * 1024 * 1024
            ),
        )(
            *[
                pltpu.with_memory_space_constraint(array, pltpu.HBM)
                for array in (
                    features, hub_block, hub_slot, neighbours.T, counts.reshape(1, -1), halo_send.reshape(-1), weight,
                    bias.reshape(1, -1),
                )
            ]
        )

    both = ("grp", "loc")
    return jax.shard_map(
        on_device,
        mesh=mesh,
        in_specs=(P(both, None), P(None, both), P(both), P(both, None), P(both), P(both, None), P(), P()),
        out_specs=P(both, None),
        check_vma=False,
    )
```

```python
import functools

import jax
import jax.numpy as jnp
from jax import lax
from jax.experimental import pallas as pl
from jax.experimental.pallas import tpu as pltpu
from jax.sharding import PartitionSpec as P

BF = jnp.bfloat16
F32 = jnp.float32
LANES = 128


def flip(index, mask, count):
    result = index
    bit = 1
    while bit < count:
        if mask & bit:
            result = result + bit * (1 - 2 * ((index // bit) % 2))
        bit *= 2
    return result


def send_order(count):
    near = [off for off in range(2, count) if bin(off >> 1).count("1") == 1]
    far = [off for off in range(2, count) if bin(off >> 1).count("1") > 1]
    near.sort(key=lambda off: (off & 1, off))
    return near[:2] + [1] + near[2:] + far


def dot(a, b):
    return jnp.dot(a, b, preferred_element_type=F32)


def dot_nt(a, b):
    return lax.dot_general(a, b, (((1,), (1,)), ((), ())), preferred_element_type=F32)


def split(x):
    high = x.astype(BF)
    return high, (x - high.astype(F32)).astype(BF)


def onehot(mask):
    return jnp.where(mask, 1.0, 0.0).astype(BF)


def iota(shape, dim):
    return lax.broadcasted_iota(jnp.int32, shape, dim)


def kernel(
    n_grp, n_loc,
    feat_hbm, hub_hbm, slot_hbm, nbr_hbm, cnt_hbm, halo_hbm, w_hbm, bias_hbm,
    out_ref,
    feat_ref, hub_ref, slot_ref, nbr_ref, cnt_ref, halo_ref, w_ref, bias_ref, loaded,
    near, go, fh, ph, pl_, prod, table, base, acc, adj_own, adj, codes, lows, outgoing, recv, mine, pair_in, part, part_in, spread, spread_in,
    inv, wh, wl,
    halo_s, halo_r, pair_s, pair_r, grp_s, grp_r, loc_s, loc_r,
):
    grp = lax.axis_index("grp")
    me = lax.axis_index("loc")
    rows, width = feat_hbm.shape
    chunk = outgoing.shape[3]
    listed = outgoing.shape[2] * chunk
    slots = nbr_ref.shape[0]
    hub_dev = slot_ref.shape[0]
    levels = rows // LANES + n_loc * listed // LANES
    per_block = 256 // slots
    blocks = rows // per_block

    def all_of(ref, count, send_sem, recv_sem):
        return pltpu.make_async_remote_copy(
            src_ref=ref.at[0:count], dst_ref=ref.at[0:count], send_sem=send_sem, recv_sem=recv_sem,
            device_id={"loc": flip(me, 1, n_loc)}, device_id_type=pl.DeviceIdType.MESH,
        )

    order = send_order(n_loc)
    early, late, held = order[:2], order[2:-1], order[-1]

    halo_load, left_load, hub_load, nbr_load, cnt_load, w_load, bias_load, slot_load, right_load = [
        pltpu.make_async_copy(source, target, loaded.at[number])
        for number, (source, target) in enumerate((
            (halo_hbm, halo_ref), (feat_hbm.at[:, 0:LANES], feat_ref.at[0]), (hub_hbm, hub_ref), (nbr_hbm, nbr_ref),
            (cnt_hbm, cnt_ref), (w_hbm, w_ref), (bias_hbm, bias_ref), (slot_hbm, slot_ref),
            (feat_hbm.at[:, LANES:], feat_ref.at[1]),
        ))
    ]
    for load in (halo_load, left_load, right_load, w_load, nbr_load, cnt_load):
        load.start()

    barrier = pltpu.get_barrier_semaphore()
    for off in range(1, n_loc):
        pl.semaphore_signal(
            barrier, inc=1, device_id={"loc": flip(me, off, n_loc)}, device_id_type=pl.DeviceIdType.MESH
        )


    def times_weight(x_high, x_low):
        return dot(x_high, wh[...]) + dot(x_low, wh[...]) + dot(x_high, wl[...])

    def whole(ref):
        return jnp.concatenate([ref[0], ref[1]], axis=1)

    def gather(source, peer, target):
        first = peer * listed

        def rows_of(step, carry):
            at = first + step * chunk
            for inner in range(chunk):
                row = halo_ref[at + inner]
                for side in range(2):
                    target[side, step, inner:inner + 1, :] = source[side, pl.ds(row, 1), :]
            return carry

        lax.fori_loop(0, listed // chunk, rows_of, 0)

    def halo_copy(off):
        return pltpu.make_async_remote_copy(
            src_ref=outgoing.at[off],
            dst_ref=recv.at[me],
            send_sem=halo_s.at[off],
            recv_sem=halo_r.at[off],
            device_id={"loc": flip(me, off, n_loc)},
            device_id_type=pl.DeviceIdType.MESH,
        )

    def held_copy(side):
        return pltpu.make_async_remote_copy(
            src_ref=outgoing.at[held, side],
            dst_ref=recv.at[me, side],
            send_sem=halo_s.at[held * (1 - side)],
            recv_sem=halo_r.at[held * (1 - side)],
            device_id={"loc": flip(me, held, n_loc)},
            device_id_type=pl.DeviceIdType.MESH,
        )

    core = me % 2
    pair_copy = pltpu.make_async_remote_copy(
        src_ref=mine.at[1 - core], dst_ref=pair_in, send_sem=pair_s, recv_sem=pair_r,
        device_id={"loc": flip(me, 1, n_loc)}, device_id_type=pl.DeviceIdType.MESH,
    )

    def grp_copy(off):
        target = (grp + off) % n_grp
        return pltpu.make_async_remote_copy(
            src_ref=part.at[target],
            dst_ref=part_in.at[off],
            send_sem=grp_s,
            recv_sem=grp_r,
            device_id={"grp": target},
            device_id_type=pl.DeviceIdType.MESH,
        )

    def loc_copy(off):
        target = flip(me, off, n_loc)
        return pltpu.make_async_remote_copy(
            src_ref=spread.at[target // 2],
            dst_ref=spread_in.at[off // 2],
            send_sem=loc_s,
            recv_sem=loc_r,
            device_id={"loc": target},
            device_id_type=pl.DeviceIdType.MESH,
        )

    word = n_loc - 1

    @pl.when(me == word - 1)
    def _():
        pl.semaphore_wait(barrier, n_loc - 1)
        pl.semaphore_signal(near, inc=1, device_id={"loc": word}, device_id_type=pl.DeviceIdType.MESH)
        for off in range(1, n_grp):
            pl.semaphore_signal(
                barrier, inc=1, device_id={"grp": (grp + off) % n_grp, "loc": word},
                device_id_type=pl.DeviceIdType.MESH,
            )

    halo_load.wait()
    left_load.wait()
    right_load.wait()
    first, second = early
    gather(feat_ref, flip(me, first, n_loc), outgoing.at[first])

    @pl.when(jnp.logical_and(me > 1, me < word - 1))
    def _():
        pl.semaphore_wait(barrier, n_loc - 1)

    @pl.when(me == word)
    def _():
        pl.semaphore_wait(near, 1)

    def send_early(off, when):
        @pl.when(when)
        def _():
            halo_copy(off).start()

    send_early(first, me > 1)
    gather(feat_ref, flip(me, second, n_loc), outgoing.at[second])
    send_early(second, me > 1)
    for load in (hub_load, bias_load, slot_load):
        load.start()

    w_load.wait()
    w_high, w_low = split(w_ref[...])
    wh[...] = w_high
    wl[...] = w_low
    high, low = split(whole(feat_ref))
    fh[...] = high
    product = times_weight(high, low)
    for side in range(2):
        prod[side] = product[:, side * LANES:(side + 1) * LANES]
    p_high, p_low = split(product)
    ph[...] = p_high
    pl_[...] = p_low

    @pl.when(me <= 1)
    def _():
        pl.semaphore_wait(barrier, n_loc - 1)

    for off in early:
        send_early(off, me <= 1)

    nbr_load.wait()
    cnt_load.wait()
    slot = nbr_ref[...]
    used = iota((slots, rows), 0) < jnp.broadcast_to(cnt_ref[...], (slots, rows))
    table[:, 0:slots] = jnp.transpose(jnp.where(used, slot, -1))
    flat = jnp.concatenate(
        [table[pl.ds(vertex, blocks, stride=per_block), 0:slots] for vertex in range(per_block)], axis=1
    )
    level = jnp.where(flat < 0, -1, lax.shift_right_logical(flat, 7))
    codes[...] = level * per_block + iota((blocks, 256), 1) // slots
    lows[...] = flat & (LANES - 1)
    inv[...] = 1.0 / jnp.transpose(jnp.broadcast_to(cnt_ref[...].astype(F32), (LANES, rows)))

    for off in late:
        gather(prod, flip(me, off, n_loc), outgoing.at[off])
        halo_copy(off).start()
    gather(prod, flip(me, held, n_loc), outgoing.at[held])
    gather(prod, me, recv.at[me])

    hub_load.wait()
    product = dot(hub_ref[...], fh[...])
    for side in range(2):
        mine[side] = jnp.concatenate(
            [product[owner * hub_dev:(owner + 1) * hub_dev] for owner in range(side, n_grp * n_loc, 2)], axis=0
        )
    pair_copy.start()

    @pl.when(me == word)
    def _():
        pl.semaphore_wait(barrier, n_loc - 1 + n_grp - 1)
        for off in range(1, n_loc):
            pl.semaphore_signal(
                go, inc=1, device_id={"loc": flip(me, off, n_loc)}, device_id_type=pl.DeviceIdType.MESH
            )
        pl.semaphore_signal(go, inc=1)


    group = 8
    own = rows // 256

    def build(step, carry):
        for inner in range(group):
            block = step * group + inner
            code = codes[pl.ds(block, 1), :]
            spot = lows[pl.ds(block, 1), :]
            left = onehot(iota((levels * per_block, 256), 0) == code)
            right = onehot(iota((LANES, 256), 0) == spot)
            counted = dot_nt(left, right).astype(BF)
            at = pl.ds(pl.multiple_of(block * per_block, per_block), per_block)
            for tile in range(levels):
                piece = counted[tile * per_block:(tile + 1) * per_block]
                if tile < 2 * own:
                    adj_own[at, tile * LANES:(tile + 1) * LANES] = piece
                else:
                    adj[tile - 2 * own, at, :] = piece
        return carry

    steps = blocks // group
    lax.fori_loop(0, steps // 4, build, 0)
    pair_copy.wait_recv()
    part[...] = (mine[core] + pair_in[...]).reshape(part.shape)
    pl.semaphore_wait(go, 1)
    for off in range(1, n_grp):
        grp_copy(off).start()
    lax.fori_loop(steps // 4, steps, build, 0)
    acc[...] = dot(adj_own[...], ph[...]) + dot(adj_own[...], pl_[...])

    all_of(part_in, n_grp - 1, grp_s, grp_r).wait_recv()
    group_sum = part[grp]
    for off in range(1, n_grp):
        group_sum = group_sum + part_in[off]
    group_sum = times_weight(*split(group_sum))
    if 2 * hub_dev < spread.shape[1]:
        spread[...] = jnp.zeros_like(spread)
    for owner in range(n_loc // 2):
        own_rows = group_sum[owner * hub_dev:(owner + 1) * hub_dev]
        spread[owner, 0:hub_dev, :] = own_rows[:, 0:width // 2]
        spread[owner, hub_dev:2 * hub_dev, :] = own_rows[:, width // 2:]
    for off in range(2, n_loc, 2):
        loc_copy(off).start()
    for side in range(2):
        held_copy(side).start()

    def take(off):
        peer = flip(me, off, n_loc)
        got = jnp.concatenate([recv[peer, side].reshape(listed, LANES) for side in range(2)], axis=1)
        if off in early:
            got = times_weight(*split(got))
        r_high, r_low = split(got)
        column = adj[peer]
        return dot(jnp.concatenate([column, column], axis=1), jnp.concatenate([r_high, r_low], axis=0))

    slot_load.wait()
    bias_load.wait()
    lane = iota((1, LANES), 1)
    target_row = jnp.full((1, LANES), -1, jnp.int32)
    for hub in range(hub_dev):
        target_row = jnp.where(lane == hub, slot_ref[hub], target_row)
    here = onehot(iota((rows, LANES), 0) == target_row)

    acc[...] += take(0)
    for off in [1] + early + late[1:]:
        halo_copy(off).wait_recv()
        acc[...] += take(off)

    scale = inv[...]
    base[...] = acc[...] * jnp.concatenate([scale, scale], axis=1) + (whole(prod) + bias_ref[...])

    hubs = spread[me // 2]
    all_of(spread_in, n_loc // 2 - 1, loc_s, loc_r).wait_recv()
    for off in range(2, n_loc, 2):
        hubs = hubs + spread_in[off // 2]
    hubs = jnp.concatenate([hubs[0:hub_dev], hubs[hub_dev:2 * hub_dev]], axis=1)
    hubs = jnp.concatenate([hubs, jnp.zeros((LANES - hub_dev, width), F32)], axis=0)
    base[...] += dot(jnp.concatenate([here, here], axis=1), jnp.concatenate(split(hubs), axis=0))

    peer = flip(me, held, n_loc)
    parts = [slice(part * rows // 2, (part + 1) * rows // 2) for part in range(2)]
    for side in range(2):
        lanes = slice(side * LANES, (side + 1) * LANES)
        held_copy(side).wait_recv()
        pair = jnp.concatenate(split(recv[peer, side].reshape(listed, LANES)), axis=0)
        for at in parts:
            column = adj[peer, at, :]
            last = dot(jnp.concatenate([column, column], axis=1), pair)
            out_ref[at, lanes] = jnp.maximum(last * inv[at, :] + base[at, lanes], 0.0)

    for off in order[:-1]:
        halo_copy(off).wait_send()
    for side in range(2):
        held_copy(side).wait_send()
    all_of(spread_in, n_loc // 2 - 1, loc_s, loc_r).wait_send()
    pair_copy.wait_send()
    all_of(part_in, n_grp - 1, grp_s, grp_r).wait_send()


def solution(mesh):
    n_grp, n_loc = mesh.shape["grp"], mesh.shape["loc"]

    def on_device(features, hub_block, hub_slot, neighbours, counts, halo_send, weight, bias):
        rows, width = features.shape
        slots = neighbours.shape[1]
        listed = halo_send.shape[1]
        chunk = 64
        hubs = hub_block.shape[0]
        blocks = rows // (256 // slots)
        padded = -(-2 * hub_slot.shape[0] // 8) * 8
        vmem = pl.BlockSpec(memory_space=pltpu.VMEM)
        far = pl.BlockSpec(memory_space=pltpu.HBM)
        sem = pltpu.SemaphoreType.DMA
        return pl.pallas_call(
            functools.partial(kernel, n_grp, n_loc),
            out_shape=jax.ShapeDtypeStruct((rows, width), F32),
            in_specs=[far] * 8,
            out_specs=vmem,
            scratch_shapes=[
                pltpu.VMEM((2, rows, LANES), F32),
                pltpu.VMEM(hub_block.shape, BF),
                pltpu.SMEM(hub_slot.shape, jnp.int32),
                pltpu.VMEM((slots, rows), jnp.int32),
                pltpu.VMEM((1, rows), jnp.int32),
                pltpu.SMEM((halo_send.size,), jnp.int32),
                pltpu.VMEM(weight.shape, F32),
                pltpu.VMEM((1, width), F32),
                sem((9,)),
                pltpu.SemaphoreType.REGULAR,
                pltpu.SemaphoreType.REGULAR,
                pltpu.VMEM((rows, width), BF),
                pltpu.VMEM((rows, width), BF),
                pltpu.VMEM((rows, width), BF),
                pltpu.VMEM((2, rows, LANES), F32),
                pltpu.VMEM((rows, LANES), jnp.int32),
                pltpu.VMEM((rows, width), F32),
                pltpu.VMEM((rows, width), F32),
                pltpu.VMEM((rows, rows), BF),
                pltpu.VMEM((n_loc, rows, LANES), BF),
                pltpu.VMEM((blocks, 256), jnp.int32),
                pltpu.VMEM((blocks, 256), jnp.int32),
                pltpu.VMEM((n_loc, 2, listed // chunk, chunk, LANES), F32),
                pltpu.VMEM((n_loc, 2, listed // chunk, chunk, LANES), F32),
                pltpu.VMEM((2, hubs // 2, width), F32),
                pltpu.VMEM((hubs // 2, width), F32),
                pltpu.VMEM((n_grp, hubs // n_grp // 2, width), F32),
                pltpu.VMEM((n_grp, hubs // n_grp // 2, width), F32),
                pltpu.VMEM((n_loc // 2, padded, width // 2), F32),
                pltpu.VMEM((n_loc // 2, padded, width // 2), F32),
                pltpu.VMEM((rows, LANES), F32),
                pltpu.VMEM(weight.shape, BF),
                pltpu.VMEM(weight.shape, BF),
                sem((n_loc,)), sem((n_loc,)), sem, sem, sem, sem, sem, sem,
            ],
            compiler_params=pltpu.CompilerParams(
                collective_id=0, has_side_effects=True, vmem_limit_bytes=48 * 1024 * 1024
            ),
        )(
            *[
                pltpu.with_memory_space_constraint(array, pltpu.HBM)
                for array in (
                    features, hub_block, hub_slot, neighbours.T, counts.reshape(1, -1), halo_send.reshape(-1), weight,
                    bias.reshape(1, -1),
                )
            ]
        )

    both = ("grp", "loc")
    return jax.shard_map(
        on_device,
        mesh=mesh,
        in_specs=(P(both, None), P(None, both), P(both), P(both, None), P(both), P(both, None), P(), P()),
        out_specs=P(both, None),
        check_vma=False,
    )
```
